512 devices in a mesh: dp: 8 (over x, core), expert: 64 (over y, z).
Axes of the slice: x: 4, y: 8, z: 8, core: 2. Of those that a mesh axis runs over, the one named last changes fastest.
Arguments:
- q_latent: bfloat16 [2048, 16, 576], P(('expert', 'dp')), may hold values from -48 to 48
- latent_cache: bfloat16 [2048, 512, 576], P(('expert', 'dp')), may hold values from -10 to 10
- lengths: int32 [2048], P(('expert', 'dp')), may hold values from 2 to 512
- residual: bfloat16 [2048, 2048], P(('expert', 'dp')), may hold values from -6 to 6
- adapter_ids: int32 [2048], P(('expert', 'dp')), may hold values from 0 to 127
- value_out: bfloat16 [8192, 2048], P('expert'), may hold values from -0.0625 to 0.0625
- adapter_down: bfloat16 [8192, 2048], P('expert'), may hold values from -0.0625 to 0.0625
- adapter_up_factors: bfloat16 [2048, 2048], P('expert'), may hold values from -1.5 to 1.5
- norm_gain: bfloat16 [2048], replicated, may hold values from 0.099609375 to 1.8984375
- expert_ids: int32 [2048, 6], P('expert'), may hold values from 0 to 63, all different within a row; in each aligned block of 32 rows (0 to 31, 32 to 63, ...) at most 8 rows name the same one
- gate_weights: float32 [2048, 6], P('expert'), may hold values from 0.05 to 0.5
- w_gate: bfloat16 [64, 2048, 1024], P('expert', None, 'dp'), may hold values from -0.125 to 0.125
- w_up: bfloat16 [64, 2048, 1024], P('expert', None, 'dp'), may hold values from -0.125 to 0.125
- w_down: bfloat16 [64, 2048, 1024], P('expert', None, 'dp'), may hold values from -0.1875 to 0.1875
Outputs:
- layer_out: bfloat16 [2048, 2048], P(('expert', 'dp'))
The draws below stay inside these ranges and needn't reach their ends.
Inputs may be any that keep to these rules, and one draw needn't show every extreme that they name: `expert_ids`: each row names 6 different experts. Requests e * 32 to e * 32 + 31 form aligned blocks; in each block no expert is named by more than 8 rows, and in some block an expert is named by exactly 8 rows.
All inputs are finite; a program needn't handle non-finite values.
Results may differ from the reference program's by a relative error of at most 0.008.
Values may be sent and summed in bfloat16 or wider, within the bound.
No kernel may reach another device: no remote copies, remote signals or barrier semaphores. Data moves between devices by JAX's collectives and lax.ppermute only.
A program may use at most 64 MiB of HBM per device.

```python
import math
import jax
import jax.numpy as jnp
import numpy as np
from jax import lax

D = 2048
HEADS = 16
LAT = 512
ROPE = 64
TOPK = 6
HID = 1024
ADAPTER_RANK = 16
CTX = 512
EXPERTS = 64
ADAPTER_TOTAL = 128
REQUEST_TOTAL = 2048
COLUMN = 32
MOST = 8
N_EXPERT = 64


def draw_q_latent(key, part):
    shape = (REQUEST_TOTAL, HEADS, LAT + ROPE)
    query = jnp.clip(jax.random.normal(jax.random.fold_in(key, 5), shape, jnp.float32), -5.0, 5.0)
    return query.astype(jnp.bfloat16)


def draw_latent_cache(key, part):
    shape = (REQUEST_TOTAL, CTX, LAT + ROPE)
    cache_rows = jnp.clip(jax.random.normal(jax.random.fold_in(key, 8), shape, jnp.float32), -5.0, 5.0)
    return cache_rows.astype(jnp.bfloat16)


def place_ends(result, own_key, smallest, largest):
    index_at = [jax.random.randint(jax.random.fold_in(own_key, axis), (), 0, length) for axis, length in enumerate(result.shape)]
    longest = result.shape.index(max(result.shape))
    neighbour = index_at[:longest] + [(index_at[longest] + 1) % result.shape[longest]] + index_at[longest + 1:]
    return result.at[tuple(index_at)].set(smallest).at[tuple(neighbour)].set(largest)


def levels(stream_key, dims, shards, low, top_value):
    gain, own = 1.0, jax.random.fold_in(stream_key, 6)
    for position, parts in shards:
        draws = jnp.exp(jax.random.uniform(jax.random.fold_in(own, position), (parts,), jnp.float32, low / len(shards), top_value / len(shards)))
        gain = gain * jnp.repeat(draws, dims[position] // parts).reshape([-1 if axis == position else 1 for axis in range(len(dims))])
    return gain


def rank_bounds(count, slope):
    loads = [(1 << 20) // math.isqrt(standing ** slope) + 1 for standing in range(1, count + 1)]
    spread = 1 + sum(loads) // (1 << 30)
    return np.cumsum(np.array([max(1, weight // spread) for weight in loads]))


def skewed_ids(rng, extent, count, slope):
    table = rank_bounds(count, slope)
    lot = jax.random.randint(jax.random.fold_in(rng, 1), extent, 0, int(table[count - 1]))
    grade = jnp.searchsorted(jnp.asarray(table, jnp.int32), lot, side="right")
    return jax.random.permutation(jax.random.fold_in(rng, 2), count)[grade].astype(jnp.int32)


def deal_out(key, own, number, rows, count, top, most, skew):
    ranking = jax.random.permutation(key, count)
    crowded, usual = shares(count, rows * top, most, skew, True), shares(count, rows * top, most, skew, False)
    places = jnp.arange(count)

    def named(tallies, rotation):
        used = int((tallies > 0).sum())
        fixed = max(1, used // 4)
        passed = fixed + (places - fixed + rotation * (used - fixed)) % max(1, count - fixed)
        return jnp.zeros((count,), jnp.int32).at[ranking[jnp.where(places < fixed, places, passed)]].set(jnp.asarray(tallies, jnp.int32))

    tallies = jnp.where(number % 4 == 0, named(crowded, number // 4), named(usual, number - number // 4 - 1))
    mixed = jax.random.permutation(jax.random.fold_in(own, 3), count)
    giver, sink = mixed[0:count // 2 * 2:2], mixed[1:count // 2 * 2:2]
    slack = jnp.minimum(tallies[giver] - 1, most - tallies[sink]) // 2
    slack = jnp.where((giver == ranking[0]) | (sink == ranking[0]) | (tallies[sink] == 0), 0, jnp.maximum(slack, 0))
    passed = jax.random.randint(jax.random.fold_in(own, 4), (count // 2,), 0, 1 << 20) % (slack + 1)
    tallies = tallies.at[giver].add(-passed).at[sink].add(passed)
    items = jnp.searchsorted(jnp.cumsum(tallies), jnp.arange(rows * top), side="right").astype(jnp.int32)
    grid = items.reshape(top, rows).T
    grid = grid[jax.random.permutation(jax.random.fold_in(own, 1), rows)]
    rotation = jax.random.randint(jax.random.fold_in(own, 2), (rows, 1), 0, top)
    return jnp.take_along_axis(grid, (jnp.arange(top)[None, :] + rotation) % top, axis=1)


def shares(number_of, total, bound, skew, full):
    portions = [(1 << 20) // math.isqrt(standing ** skew) + 1 for standing in range(1, number_of + 1)]
    largest = bound if full else min(bound, max(-(-total // number_of), total * portions[0] // sum(portions)))
    least = 1 if total - largest >= number_of - 1 else 0
    holding, rest = [largest] + [least] * (number_of - 1), total - largest - least * (number_of - 1)
    while rest > 0:
        movable = [i for i in range(1, number_of) if holding[i] < largest] or [i for i in range(1, number_of) if holding[i] < bound]
        whole, left = sum([portions[i] for i in movable]), rest
        for i in movable:
            addition = min(bound - holding[i], max(1, left * portions[i] // whole), rest)
            holding[i] = holding[i] + addition
            rest = rest - addition
    return np.array(holding)


def scatter_about(key, dims, spread, reach, cuts=(), kind=jnp.bfloat16):
    drawn = jax.random.normal(key, dims, jnp.float32) * spread
    if len(cuts) > 0:
        drawn = levels(key, dims, cuts, -0.22, 0.18) * drawn
    return jnp.clip(drawn, min=-reach, max=reach).astype(kind)


def setup_inputs(seed: int = 0) -> dict:
    key_of = jax.random.split(jax.random.key(seed), 15)
    q_latent = draw_q_latent(jax.random.fold_in(key_of[14], 71), 0)
    latent_cache = draw_latent_cache(jax.random.fold_in(key_of[14], 71), 0)
    lengths = place_ends(jax.random.randint(key_of[2], (REQUEST_TOTAL,), 2, CTX + 1), jax.random.fold_in(key_of[2], 1), 2, CTX).astype(jnp.int32)
    residual = scatter_about(key_of[3], (REQUEST_TOTAL, D), 1.0, 6.0, ((0, 512),))
    adapter_ids = place_ends(skewed_ids(key_of[4], (REQUEST_TOTAL,), ADAPTER_TOTAL, 2), jax.random.fold_in(key_of[4], 3), 0, ADAPTER_TOTAL - 1).astype(jnp.int32)
    value_out = scatter_about(key_of[5], (HEADS * LAT, D), (HEADS * LAT) ** -0.5, 0.0625, ((0, 64),))
    adapter_down = scatter_about(key_of[6], (HEADS * LAT, ADAPTER_TOTAL * ADAPTER_RANK), (HEADS * LAT) ** -0.5, 0.0625, ((0, 64),))
    adapter_up_factors = scatter_about(key_of[7], (ADAPTER_TOTAL * ADAPTER_RANK, D), ADAPTER_RANK ** -0.5, 1.5, ((0, 64),))
    norm_gain = jnp.clip(1.0 + 0.18 * jax.random.normal(key_of[8], (D,), jnp.float32), 0.099609375, 1.8984375).astype(jnp.bfloat16)
    expert_ids_keys = jax.random.split(jax.random.fold_in(key_of[9], 1), REQUEST_TOTAL // COLUMN)
    expert_ids_turns = jax.random.permutation(jax.random.fold_in(key_of[9], 3), REQUEST_TOTAL // COLUMN)
    expert_ids = jax.vmap(lambda own, number: deal_out(jax.random.fold_in(key_of[9], 2), own, number, COLUMN, EXPERTS, TOPK, MOST, 2))(expert_ids_keys, expert_ids_turns).reshape((REQUEST_TOTAL, TOPK))
    gate_weights = jnp.clip(jnp.exp(math.log(0.5) - 2.3025851 * jax.random.uniform(key_of[10], (REQUEST_TOTAL, TOPK), jnp.float32) ** levels(key_of[10], (REQUEST_TOTAL, TOPK), ((0, 64),), -0.2, 0.2)), 0.05, 0.5)
    w_gate = scatter_about(key_of[11], (EXPERTS, D, HID), D ** -0.5, 0.125, ((0, 64), (2, 8)))
    w_up = scatter_about(key_of[12], (EXPERTS, D, HID), D ** -0.5, 0.125, ((0, 64), (2, 8)))
    w_down = scatter_about(key_of[13], (EXPERTS, D, HID), HID ** -0.5, 0.1875, ((0, 64), (2, 8)))
    return {"q_latent": q_latent, "latent_cache": latent_cache, "lengths": lengths, "residual": residual, "adapter_ids": adapter_ids, "value_out": value_out, "adapter_down": adapter_down, "adapter_up_factors": adapter_up_factors, "norm_gain": norm_gain, "expert_ids": expert_ids, "gate_weights": gate_weights, "w_gate": w_gate, "w_up": w_up, "w_down": w_down}


SOFTMAX_SCALE = 192.0 ** (-0.5)
ADAPTER_SCALE = 2.0
EPSILON = 1e-06

def attend_one(query, latent_rows, length):
    scores = jnp.dot(query, latent_rows.T, preferred_element_type=jnp.float32) * SOFTMAX_SCALE
    valid_mask = jnp.arange(latent_rows.shape[0], dtype=jnp.int32) < length
    scores = jnp.where(valid_mask[None, :], scores, -1e+30)
    row_max = lax.optimization_barrier(jnp.max(scores, axis=1, keepdims=True))
    raised = jnp.exp(scores - row_max)
    weights_bf = (raised / lax.optimization_barrier(jnp.sum(raised, axis=1, keepdims=True))).astype(jnp.bfloat16)
    return jnp.dot(weights_bf, latent_rows[:, :LAT], preferred_element_type=jnp.float32).astype(jnp.bfloat16)

def reference(q_latent, latent_cache, lengths, residual, adapter_ids, value_out, adapter_down, adapter_up_factors, norm_gain, expert_ids, gate_weights, w_gate, w_up, w_down):
    latent_out = lax.map(lambda packed: attend_one(packed[0], packed[1], packed[2]), (q_latent, latent_cache, lengths))
    latent_out = latent_out.reshape(REQUEST_TOTAL, HEADS * LAT)
    base_output = jnp.dot(latent_out, value_out, preferred_element_type=jnp.float32)
    down_projected_rows = jnp.dot(latent_out, adapter_down, preferred_element_type=jnp.float32).reshape(REQUEST_TOTAL, ADAPTER_TOTAL, ADAPTER_RANK)
    chosen_adapters = adapter_ids[:, None] == jnp.arange(ADAPTER_TOTAL, dtype=jnp.int32)[None, :]
    adapter_down_rows = lax.optimization_barrier(jnp.sum(jnp.where(chosen_adapters[:, :, None], down_projected_rows, 0.0), axis=1))
    adapter_scaled_output = (ADAPTER_SCALE * adapter_down_rows).astype(jnp.bfloat16)
    spread_rows = jnp.where(chosen_adapters[:, :, None], adapter_scaled_output[:, None, :], jnp.zeros((), jnp.bfloat16)).reshape(REQUEST_TOTAL, ADAPTER_TOTAL * ADAPTER_RANK)
    adapter_up_rows = jnp.dot(spread_rows, adapter_up_factors, preferred_element_type=jnp.float32)
    residual_flow = residual.astype(jnp.float32) + base_output + adapter_up_rows
    inverse_rms = lax.rsqrt(lax.optimization_barrier(jnp.mean(residual_flow * residual_flow, axis=1, keepdims=True)) + EPSILON)
    normed = (residual_flow * inverse_rms * norm_gain.astype(jnp.float32)).astype(jnp.bfloat16)
    load_bound = N_EXPERT * MOST
    padded = jnp.concatenate([normed, jnp.zeros((1, D), jnp.bfloat16)], axis=0)

    def one_expert(running, expert_index):
        hit_mask = expert_ids == expert_index
        member = jnp.any(hit_mask, axis=1)
        gate_sum = lax.optimization_barrier(jnp.sum(jnp.where(hit_mask, gate_weights, 0.0), axis=1))
        row_index = jnp.nonzero(member, size=load_bound, fill_value=REQUEST_TOTAL)[0].astype(jnp.int32)
        tokens = padded[row_index]
        gate_act = jnp.dot(tokens, w_gate[expert_index], preferred_element_type=jnp.float32)
        up_act = jnp.dot(tokens, w_up[expert_index], preferred_element_type=jnp.float32)
        hidden_bf = (jax.nn.silu(gate_act) * up_act).astype(jnp.bfloat16)
        produced = lax.dot_general(hidden_bf, w_down[expert_index], (((1,), (1,)), ((), ())), preferred_element_type=jnp.float32)
        gate_rows = jnp.concatenate([gate_sum, jnp.zeros((1,), gate_sum.dtype)])[row_index]
        running = running.at[row_index].add(gate_rows[:, None] * produced, mode='drop')
        return (running, None)
    routed, unused = lax.scan(one_expert, jnp.zeros((REQUEST_TOTAL, D), jnp.float32), jnp.arange(EXPERTS, dtype=jnp.int32))
    return (residual_flow + routed).astype(jnp.bfloat16)
```

```python
import functools

import jax
import jax.numpy as jnp
from jax import lax
from jax.sharding import Mesh
from jax.sharding import PartitionSpec as P

LAT = 512
ADAPTER_RANK = 16
EXPERT = ("expert_0", "expert_1")
EXPERT_DP = ("expert_0", "expert_1", "dp")


SOFTMAX_SCALE = 192.0 ** (-0.5)
ADAPTER_SCALE = 2.0
EPSILON = 1e-06


def copy_for_each(shard, axis):
    copies = jnp.broadcast_to(shard, (lax.axis_size(axis), *shard.shape))
    return lax.all_to_all(copies, axis, split_axis=0, concat_axis=0, tiled=True)


def joined_along(blocks, dim):
    dims = list(blocks.shape[1:])
    dims[dim] *= blocks.shape[0]
    return jnp.moveaxis(blocks, 0, dim).reshape(dims)


def gathered_copies(shard, axis, dim):
    blocks = copy_for_each(shard, axis)
    return joined_along(blocks, dim)


def one_axis_at_a_time(shard, axes):
    return functools.reduce(lax.psum, axes, shard)


def cut_along(shard, dim, count):
    dims = shard.shape
    blocks = shard.reshape(*dims[:dim], count, dims[dim] // count, *dims[dim + 1 :])
    return jnp.moveaxis(blocks, dim, 0)


def sum_at_owner(shard, axis, dim):
    blocks = cut_along(shard, dim, lax.axis_size(axis))
    arrived = lax.all_to_all(blocks, axis, split_axis=0, concat_axis=0, tiled=True)
    return arrived.sum(axis=0)


def in_one_piece(arrays, axis, dim, along):
    both = jnp.concatenate(arrays, axis=along)
    whole, at, gathered = (lax.all_gather(both, axis, axis=dim, tiled=True), 0, [])
    for a in arrays:
        gathered.append(lax.slice_in_dim(whole, at, at + a.shape[along], axis=along))
        at += a.shape[along]
    return tuple(gathered)


def summed_on_arrival(shard, axis, dim):
    blocks = cut_along(shard, dim, lax.axis_size(axis))
    arrived = lax.all_to_all(blocks, axis, split_axis=0, concat_axis=0, tiled=True)
    return arrived.astype(jnp.float32).sum(axis=0)


def attend_one(query, latent_rows, length):
    scores = (
        lax.dot_general(
            query, latent_rows, (((1,), (1,)), ((), ())), preferred_element_type=jnp.float32
        )
        * SOFTMAX_SCALE
    )
    valid_mask = jnp.arange(latent_rows.shape[0], dtype=jnp.int32) < length
    scores = jnp.where(valid_mask[None, :], scores, -1e30)
    row_max = jnp.max(scores, axis=1, keepdims=True)
    raised = jnp.exp(scores - row_max)
    weights_bf = (raised / jnp.sum(raised, axis=1, keepdims=True)).astype(jnp.bfloat16)
    return jnp.dot(weights_bf, latent_rows[:, :LAT], preferred_element_type=jnp.float32).astype(
        jnp.bfloat16
    )


def expert_rows(tokens, gate_part, up_part, down_part):
    gate_act = jnp.dot(tokens, gate_part, preferred_element_type=jnp.float32)
    up_act = jnp.dot(tokens, up_part, preferred_element_type=jnp.float32)
    hidden_bf = (jax.nn.silu(gate_act) * up_act).astype(jnp.bfloat16)
    return lax.dot_general(
        hidden_bf, down_part, (((1,), (1,)), ((), ())), preferred_element_type=jnp.float32
    )


def local(
    q_latent,
    latent_cache,
    lengths,
    residual,
    adapter_ids,
    value_out,
    adapter_down,
    adapter_up_factors,
    norm_gain,
    expert_ids,
    gate_weights,
    w_gate,
    w_up,
    w_down,
):
    requests = residual.shape[0]
    model_width = residual.shape[1]
    head_count = q_latent.shape[1]
    latent_out = jax.vmap(attend_one)(q_latent, latent_cache, lengths).reshape(
        requests, head_count * LAT
    )
    adapters = adapter_down.shape[1] // ADAPTER_RANK
    owned_count = adapter_up_factors.shape[0] // ADAPTER_RANK
    owners = lax.axis_size(EXPERT)
    depth = adapter_down.shape[0]
    sent = jnp.moveaxis(latent_out.reshape(requests, owners, depth), 1, 0)
    sent_ids = jnp.broadcast_to(
        adapter_ids.astype(jnp.bfloat16)[None, :, None], (owners, requests, depth)
    )
    arrived = lax.all_to_all(
        jnp.concatenate([sent, sent_ids], axis=1), EXPERT, split_axis=0, concat_axis=0, tiled=True
    )
    pieces = arrived.reshape(owners * 2 * requests, depth)
    group_ids = arrived[:, requests:, 0].astype(jnp.int32)
    row_ids = jnp.concatenate([group_ids, jnp.full_like(group_ids, -1)], axis=1).reshape(-1)
    down_rows = jnp.dot(pieces, adapter_down, preferred_element_type=jnp.float32).reshape(
        -1, adapters, ADAPTER_RANK
    )
    chosen = row_ids[:, None] == jnp.arange(adapters, dtype=jnp.int32)[None, :]
    lora_down = jnp.sum(jnp.where(chosen[:, :, None], down_rows, 0.0), axis=1)
    lora_down = lora_down.reshape(owners, 2 * requests, ADAPTER_RANK)[:, :requests]
    lora_down = lora_down.reshape(owners * requests, ADAPTER_RANK).T
    for axis in EXPERT:
        lora_down = copy_for_each(lora_down, axis).sum(axis=0)
    lora_scaled = (ADAPTER_SCALE * lora_down.T).astype(jnp.bfloat16)
    lora_scaled = jnp.pad(
        lora_scaled.reshape(owners, requests, ADAPTER_RANK), ((0, 0), (0, requests), (0, 0))
    ).reshape(-1, ADAPTER_RANK)
    owned = lax.axis_index(EXPERT) * owned_count + jnp.arange(owned_count, dtype=jnp.int32)
    spread_rows = jnp.where(
        (row_ids[:, None] == owned[None, :])[:, :, None],
        lora_scaled[:, None, :],
        jnp.zeros((), jnp.bfloat16),
    ).reshape(-1, owned_count * ADAPTER_RANK)
    partial = jnp.dot(pieces, value_out, preferred_element_type=jnp.float32) + jnp.dot(
        spread_rows, adapter_up_factors, preferred_element_type=jnp.float32
    )
    partial = partial.reshape(owners, 2 * requests, model_width)[:, :requests]
    attention = (
        lax.all_to_all(
            partial.astype(jnp.bfloat16), EXPERT, split_axis=0, concat_axis=0, tiled=True
        )
        .astype(jnp.float32)
        .sum(axis=0)
    )
    residual_flow = residual.astype(jnp.float32) + attention
    inverse_rms = lax.rsqrt(
        jnp.mean(residual_flow * residual_flow, axis=1, keepdims=True) + EPSILON
    )
    normed = (residual_flow * inverse_rms * norm_gain.astype(jnp.float32)).astype(jnp.bfloat16)
    column = gathered_copies(normed, "dp", 0)
    tokens = column.shape[0]
    top_count = expert_ids.shape[1]
    experts = lax.axis_size(EXPERT) * w_gate.shape[0]
    share_size = max(1, 2 * requests * top_count // experts)
    dp_count = lax.axis_size("dp")
    slot_count = share_size * dp_count
    position = lax.axis_index("dp")
    member = expert_ids[:, :, None] == jnp.arange(experts, dtype=jnp.int32)[None, None, :]
    flat_hits = member.reshape(tokens * top_count, experts).astype(jnp.int32)
    slot_rank = jnp.sum((jnp.cumsum(flat_hits, axis=0) - 1) * flat_hits, axis=1).reshape(
        tokens, top_count
    )
    placed = member[:, :, :, None] & (
        slot_rank[:, :, None, None] == jnp.arange(slot_count, dtype=jnp.int32)[None, None, None, :]
    )
    routing = jnp.any(placed, axis=1).reshape(tokens, experts * slot_count)
    combine = jnp.sum(jnp.where(placed, gate_weights[:, :, None, None], 0.0), axis=1).reshape(
        tokens, experts * slot_count
    )
    routing_rows = routing.T.astype(jnp.bfloat16)
    portion = lax.dynamic_slice_in_dim(
        routing_rows.reshape(experts, slot_count, tokens), position * share_size, share_size, 1
    ).reshape(experts * share_size, tokens)
    outgoing = (
        jnp.dot(portion, column, preferred_element_type=jnp.float32)
        .astype(jnp.bfloat16)
        .reshape(experts, share_size, model_width)
    )
    own_share = lax.all_to_all(outgoing, EXPERT, split_axis=0, concat_axis=0, tiled=True)
    weights_share = lax.dynamic_slice_in_dim(
        combine.reshape(tokens, experts, slot_count), position * share_size, share_size, 2
    ).reshape(tokens, experts * share_size)
    share_rows = own_share.reshape(experts * share_size, model_width)
    pieces_now = in_one_piece((w_gate, w_up, w_down), "dp", 2, 0)
    result = expert_rows(share_rows, pieces_now[0][0], pieces_now[1][0], pieces_now[2][0])
    returned = lax.all_to_all(
        result.reshape(experts, share_size, model_width).astype(jnp.bfloat16),
        EXPERT,
        split_axis=0,
        concat_axis=0,
        tiled=True,
    ).astype(jnp.float32)
    routed_column = jnp.dot(
        weights_share,
        returned.reshape(experts * share_size, model_width),
        precision=lax.Precision.HIGHEST,
        preferred_element_type=jnp.float32,
    )
    routed_sum = summed_on_arrival(routed_column.astype(jnp.bfloat16), "dp", 0)
    return (residual_flow + routed_sum).astype(jnp.bfloat16)


def solution(mesh):
    split = Mesh(mesh.devices.reshape(mesh.shape["dp"], 8, 8), ("dp", "expert_0", "expert_1"))
    in_specs = (
        P(EXPERT_DP, None, None),
        P(EXPERT_DP, None, None),
        P(EXPERT_DP),
        P(EXPERT_DP, None),
        P(EXPERT_DP),
        P(EXPERT, None),
        P(EXPERT, None),
        P(EXPERT, None),
        P(),
        P(EXPERT, None),
        P(EXPERT, None),
        P(EXPERT, None, "dp"),
        P(EXPERT, None, "dp"),
        P(EXPERT, None, "dp"),
    )
    out_specs = P(EXPERT_DP, None)
    return jax.shard_map(local, mesh=split, in_specs=in_specs, out_specs=out_specs, check_vma=False)
```

```python
import functools

import jax
import jax.numpy as jnp
from jax import lax
from jax.experimental import pallas as pl
from jax.experimental.pallas import tpu as pltpu
from jax.sharding import Mesh
from jax.sharding import PartitionSpec as P

LAT = 512
RANK = 16
EXPERT = ("expert_0", "expert_1")
EXPERT_DP = ("expert_0", "expert_1", "dp")
CUTS = 8
SOFTMAX_SCALE = 192.0 ** (-0.5)
ADAPTER_SCALE = 2.0
EPSILON = 1e-06
F32 = jnp.float32
BF16 = jnp.bfloat16
WHOLE = pl.BlockSpec(memory_space=pltpu.VMEM)
SCALARS = pl.BlockSpec(memory_space=pltpu.SMEM)
GRANT = pltpu.CompilerParams(vmem_limit_bytes=16 * 2**20)


def shape(dims, dtype):
    return jax.ShapeDtypeStruct(dims, dtype)


def call(kernel, outs, flops=10**7, nbytes=10**6):
    return functools.partial(
        pl.pallas_call,
        kernel,
        out_shape=outs,
        cost_estimate=pl.CostEstimate(flops=flops, bytes_accessed=nbytes, transcendentals=0),
        compiler_params=GRANT,
    )


def exchange(rows, axis):
    return lax.all_to_all(rows, axis, split_axis=0, concat_axis=0, tiled=True)


def index(dims, dim):
    return lax.broadcasted_iota(jnp.int32, dims, dim)


def one_hot(dims, hit):
    return jnp.where(hit(index(dims, 0), index(dims, 1)), 1.0, 0.0).astype(BF16)


def dot(a, b):
    return jnp.dot(a, b, preferred_element_type=F32)


def dot_t(a, b):
    return lax.dot_general(a, b, (((1,), (1,)), ((), ())), preferred_element_type=F32)


def attend_kernel(lengths, ids, query, cache, out, held):
    step, n = pl.program_id(0), pl.num_programs(0)
    heads = query.shape[1]
    scores = dot(query[0], cache[0]) * SOFTMAX_SCALE
    valid = index(scores.shape, 1) < lengths[step]
    scores = jnp.where(valid, scores, -1e30)
    raised = jnp.exp(scores - jnp.max(scores, axis=1, keepdims=True))
    weights = (raised / jnp.sum(raised, axis=1, keepdims=True)).astype(BF16)
    latents = dot_t(weights, cache[0, :LAT, :])
    lanes = out.shape[1]
    quarters = LAT // lanes
    for k in range(quarters):
        at = pl.multiple_of((step * quarters + k) * heads, heads)
        held[pl.ds(at, heads), :] = latents[:, k * lanes : (k + 1) * lanes].astype(BF16)

    @pl.when(step == n - 1)
    def _():
        rows, source = out.shape[0], held.shape[0]
        slots = 2 * 4

        def hit(o, c):
            owner, i = o // slots, o % slots
            want = i * (quarters * heads) + (owner % quarters) * heads + owner // quarters
            return (i < slots // 2) & (c == want)

        packed = dot(one_hot((rows, source), hit), held[...])
        i = index(packed.shape, 0) % slots
        for r in range(slots // 2):
            packed = jnp.where(i == slots // 2 + r, ids[r].astype(F32), packed)
        out[...] = packed.astype(BF16)


def attend(query, cache_t, lengths, ids, owners):
    n, heads, width = query.shape
    context = cache_t.shape[2]
    lanes = heads * LAT // owners
    return pl.pallas_call(
        attend_kernel,
        out_shape=shape((owners * 2 * n, lanes), BF16),
        grid_spec=pltpu.PrefetchScalarGridSpec(
            num_scalar_prefetch=2,
            grid=(n,),
            in_specs=[
                pl.BlockSpec((1, heads, width), lambda i, *_: (i, 0, 0)),
                pl.BlockSpec((1, width, context), lambda i, *_: (i, 0, 0)),
            ],
            out_specs=pl.BlockSpec((owners * 2 * n, lanes), lambda i, *_: (0, 0)),
            scratch_shapes=[pltpu.VMEM((n * heads * LAT // lanes, lanes), BF16)],
        ),
        cost_estimate=pl.CostEstimate(
            flops=4 * n * heads * width * context,
            bytes_accessed=2 * n * width * context,
            transcendentals=0,
        ),
        compiler_params=pltpu.CompilerParams(vmem_limit_bytes=53 * 2**20),
    )(lengths, ids, query, cache_t)


def lora_kernel(arrived, down, copies, pieces, numbers):
    rows = pieces.shape[0]
    lanes = arrived.shape[1]
    half = 4
    both = arrived[...]
    dims = (rows, 2 * rows)
    kept = dot(one_hot(dims, lambda o, c: c == (o // half) * 2 * half + o % half), both)
    named = dot(one_hot(dims, lambda o, c: c == (o // half) * 2 * half + half + o % half), both)
    kept = kept.astype(BF16)
    pieces[...] = kept
    numbers[...] = named.T[:8]
    total = jnp.zeros((rows, lanes), F32)
    group = index((rows, lanes), 1) // RANK
    own = named.astype(jnp.int32)
    for t in range(down.shape[1] // lanes):
        product = dot(kept, down[:, t * lanes : (t + 1) * lanes])
        total = total + jnp.where(own == group + t * (lanes // RANK), product, 0.0)
    shift = RANK
    while shift < lanes:
        total = total + pltpu.roll(total, shift, 1)
        shift *= 2
    turned = total.T[:RANK]
    for k in range(copies.shape[0]):
        copies[k] = turned


def resend_kernel(arrived, copies):
    total = jnp.sum(arrived[...], axis=0)
    for k in range(copies.shape[0]):
        copies[k] = total


def project_kernel(first, arrived, pieces, numbers, value, up, out):
    scaled = (ADAPTER_SCALE * jnp.sum(arrived[...], axis=0)).astype(BF16).astype(F32)
    number = numbers[:1].astype(jnp.int32)
    owned = up.shape[0] // RANK
    spread = [jnp.where(number == first[0] + k, scaled, 0.0) for k in range(owned)]
    spread = jnp.concatenate(spread, axis=0).T.astype(BF16)
    kept = pieces[...]
    homes, _, columns = out.shape
    rows = kept.shape[0]
    low = index((rows // 8, 8, columns), 1) < 4
    for pair in range(0, CUTS, 4):
        blocks = []
        for cut in range(pair, pair + 4):
            at = slice(cut * columns, (cut + 1) * columns)
            block = dot(kept, value[:, at]) + dot(spread, up[:, at])
            blocks.append(block.reshape(rows // 8, 8, columns))
        joined = []
        for a, b in (blocks[:2], blocks[2:]):
            even = jnp.where(low, a, pltpu.roll(b, 4, 1))
            odd = jnp.where(low, pltpu.roll(a, 4, 1), b)
            joined.append(jnp.stack([even, odd], axis=1).reshape(homes, 8, columns))
        both = jnp.concatenate(joined, axis=1)
        out[:, pair * 4 : (pair + 4) * 4, :] = both.astype(BF16)


def norm_kernel(arrived, residual, gain, stream, copies):
    flow = residual[...] + jnp.sum(arrived[...].astype(F32), axis=0)
    stream[...] = flow
    rows, columns = flow.shape
    squares = jnp.sum(flow * flow, axis=1, keepdims=True)
    for shift in (4, 8, 16):
        squares = squares + pltpu.roll(jnp.broadcast_to(squares, (rows, 128)), shift, 0)[:, :1]
    scale = lax.rsqrt(squares / (columns * CUTS) + EPSILON)
    normed = (flow * scale * gain[...]).astype(BF16)
    for k in range(copies.shape[0]):
        copies[k] = normed


def routes_kernel(routing, weights, pick, give):
    experts, tokens = routing.shape
    wide, long = tokens * CUTS, experts * CUTS
    to_expert = one_hot((long, experts), lambda o, c: o // CUTS == c)
    to_token = one_hot(
        (tokens, wide), lambda c, o: (o // (4 * CUTS) == c // 4) & (o % 4 == c % 4)
    )
    same = index((long, wide), 0) % CUTS == (index((long, wide), 1) // 4) % CUTS
    spread = dot(dot(to_expert, routing[...]).astype(BF16), to_token)
    pick[...] = jnp.where(same, spread, 0.0).astype(BF16)
    left = weights[...]
    for k in range(3):
        term = left.astype(BF16)
        left = left - term.astype(F32)
        spread = dot(dot(to_expert, term).astype(BF16), to_token)
        give[k] = jnp.where(same, spread, 0.0).astype(BF16)


def pick_kernel(pick, tokens, out):
    out[...] = dot(pick[...], tokens[...]).astype(BF16)


def give_kernel(give, rows, out):
    total = None
    for k in range(3):
        term = lax.dot_general(
            give[k], rows[...], (((0,), (0,)), ((), ())), preferred_element_type=F32
        )
        total = term if total is None else total + term
    out[...] = total.astype(BF16)


def ffn_kernel(rows, gate, up, down, out, gate_here, up_here, down_here, done):
    length, columns = rows.shape
    slots = length // CUTS
    parts = [slice(at, at + columns) for at in range(0, gate.shape[1], columns)]
    pairs = ((gate, gate_here), (up, up_here), (down, down_here))
    fetches = [
        [
            pltpu.make_async_copy(source.at[:, part], target.at[:, part], done.at[k, n])
            for k, (source, target) in enumerate(pairs)
        ]
        for n, part in enumerate(parts)
    ]
    for fetch in fetches:
        for copy in fetch:
            copy.start()
    apart = one_hot((length, length), lambda o, c: c == (o % slots) * CUTS + o // slots)
    apart = dot(apart, rows[...]).astype(BF16)
    tokens = jnp.concatenate(
        [apart[cut * slots : (cut + 1) * slots] for cut in range(CUTS)], axis=1
    )
    total = None
    for part, fetch in zip(parts, fetches):
        fetch[0].wait()
        gated = dot(tokens, gate_here[:, part])
        fetch[1].wait()
        raised = dot(tokens, up_here[:, part])
        acted = (gated / (1.0 + jnp.exp(-gated)) * raised).astype(BF16)
        fetch[2].wait()
        term = dot_t(acted, down_here[:, part])
        total = term if total is None else total + term
    result = total.astype(BF16)
    stacked = jnp.concatenate(
        [result[:, cut * columns : (cut + 1) * columns] for cut in range(CUTS)], axis=0
    )
    joint = one_hot((length, length), lambda o, c: c == (o % CUTS) * slots + o // CUTS)
    out[...] = dot(joint, stacked).astype(BF16)


def ffn(rows, gate, up, down):
    width, hidden = gate.shape
    slots, columns = rows.shape[0] // CUTS, rows.shape[1]
    return pl.pallas_call(
        ffn_kernel,
        out_shape=shape(rows.shape, BF16),
        in_specs=[WHOLE] + [pl.BlockSpec(memory_space=pl.ANY)] * 3,
        out_specs=WHOLE,
        scratch_shapes=[pltpu.VMEM((width, hidden), BF16)] * 3
        + [pltpu.SemaphoreType.DMA((3, hidden // columns))],
        cost_estimate=pl.CostEstimate(
            flops=6 * slots * width * hidden,
            bytes_accessed=6 * width * hidden,
            transcendentals=0,
        ),
        compiler_params=pltpu.CompilerParams(vmem_limit_bytes=50 * 2**20),
    )(rows, gate, up, down)


def final_kernel(arrived, stream, out):
    total = stream[...] + jnp.sum(arrived[...].astype(F32), axis=0)
    columns = total.shape[1]
    n = out.shape[0]
    for cut in range(CUTS):
        out[:, cut * columns : (cut + 1) * columns] = total[cut * n : (cut + 1) * n].astype(BF16)


def local(
    q_latent,
    latent_cache,
    lengths,
    residual,
    adapter_ids,
    value_out,
    adapter_down,
    adapter_up_factors,
    norm_gain,
    expert_ids,
    gate_weights,
    w_gate,
    w_up,
    w_down,
):
    requests, model_width = residual.shape
    owners = lax.axis_size(EXPERT)
    dp_count = lax.axis_size("dp")
    columns = model_width // CUTS
    group = owners * requests
    owned_count = adapter_up_factors.shape[0] // RANK
    packed = attend(q_latent, jnp.swapaxes(latent_cache, 1, 2), lengths, adapter_ids, owners)
    lanes = packed.shape[1]
    first = (lax.axis_index(EXPERT) * owned_count).astype(jnp.int32).reshape(1)
    packed, first = lax.optimization_barrier((packed, first))
    arrived = exchange(packed.reshape(owners, 2 * requests, lanes), EXPERT)
    arrived = arrived.reshape(owners * 2 * requests, lanes)
    side = lax.axis_size(EXPERT[0])
    copies, pieces, numbers = call(
        lora_kernel,
        (
            shape((side, RANK, group), F32),
            shape((group, lanes), BF16),
            shape((8, group), F32),
        ),
    )(in_specs=[WHOLE, WHOLE], out_specs=(WHOLE, WHOLE, WHOLE))(arrived, adapter_down)
    half = exchange(copies, EXPERT[0])
    copies = call(resend_kernel, shape((side, RANK, group), F32))(
        in_specs=[WHOLE], out_specs=WHOLE
    )(half)
    summed = exchange(copies, EXPERT[1])
    partial = call(project_kernel, shape((owners, CUTS * requests, columns), BF16))(
        in_specs=[SCALARS, WHOLE, WHOLE, WHOLE, WHOLE, WHOLE], out_specs=WHOLE
    )(first, summed, pieces, numbers, value_out, adapter_up_factors)
    at_home = exchange(partial, EXPERT)

    tokens, top_count = expert_ids.shape
    experts = owners * w_gate.shape[0]
    position = lax.axis_index("dp")
    member = expert_ids[:, :, None] == jnp.arange(experts, dtype=jnp.int32)[None, None, :]
    flat_hits = member.reshape(tokens * top_count, experts).astype(jnp.int32)
    slot_rank = jnp.sum((jnp.cumsum(flat_hits, axis=0) - 1) * flat_hits, axis=1).reshape(
        tokens, top_count
    )
    mine = member & (slot_rank == position)[:, :, None]
    routing = jnp.any(mine, axis=1).astype(BF16).T
    weights = jnp.sum(jnp.where(mine, gate_weights[:, :, None], 0.0), axis=1).T
    wide, long = tokens * CUTS, experts * CUTS
    pick, give = call(
        routes_kernel, (shape((long, wide), BF16), shape((3, long, wide), BF16))
    )(in_specs=[WHOLE, WHOLE], out_specs=(WHOLE, WHOLE))(routing, weights)

    def cut_rows(rows):
        return jnp.moveaxis(rows.reshape(-1, CUTS, columns), 1, 0)

    residual_cut = cut_rows(residual.astype(F32)).reshape(CUTS * requests, columns)
    gain_cut = jnp.broadcast_to(
        cut_rows(norm_gain.astype(F32)), (CUTS, requests, columns)
    ).reshape(CUTS * requests, columns)
    at_home, pick, give, residual_cut, gain_cut = lax.optimization_barrier(
        (at_home, pick, give, residual_cut, gain_cut)
    )
    stream, copies = call(
        norm_kernel,
        (shape((CUTS * requests, columns), F32), shape((dp_count, CUTS * requests, columns), BF16)),
    )(in_specs=[WHOLE, WHOLE, WHOLE], out_specs=(WHOLE, WHOLE))(at_home, residual_cut, gain_cut)
    column = exchange(copies, "dp").reshape(wide, columns)
    outgoing = call(pick_kernel, shape((long, columns), BF16))(
        in_specs=[WHOLE, WHOLE], out_specs=WHOLE
    )(pick, column)
    gathered = [lax.all_gather(w[0], "dp", axis=1, tiled=True) for w in (w_gate, w_up, w_down)]
    own_share = exchange(outgoing.reshape(experts, CUTS, columns), EXPERT).reshape(long, columns)
    result = ffn(own_share, *gathered)
    returned = exchange(result.reshape(experts, CUTS, columns), EXPERT).reshape(long, columns)
    routed = call(give_kernel, shape((wide, columns), BF16))(
        in_specs=[WHOLE, WHOLE], out_specs=WHOLE
    )(give, returned)
    terms = exchange(routed.reshape(dp_count, CUTS * requests, columns), "dp")
    return call(final_kernel, shape((requests, model_width), BF16))(
        in_specs=[WHOLE, WHOLE], out_specs=WHOLE
    )(terms, stream)


def solution(mesh):
    split = Mesh(mesh.devices.reshape(mesh.shape["dp"], 8, 8), ("dp", "expert_0", "expert_1"))
    in_specs = (
        P(EXPERT_DP, None, None),
        P(EXPERT_DP, None, None),
        P(EXPERT_DP),
        P(EXPERT_DP, None),
        P(EXPERT_DP),
        P(EXPERT, None),
        P(EXPERT, None),
        P(EXPERT, None),
        P(),
        P(EXPERT, None),
        P(EXPERT, None),
        P(EXPERT, None, "dp"),
        P(EXPERT, None, "dp"),
        P(EXPERT, None, "dp"),
    )
    out_specs = P(EXPERT_DP, None)
    return jax.shard_map(local, mesh=split, in_specs=in_specs, out_specs=out_specs, check_vma=False)
```

```python
import functools

import jax
import jax.numpy as jnp
from jax import lax
from jax.experimental import pallas as pl
from jax.experimental.pallas import tpu as pltpu
from jax.sharding import Mesh
from jax.sharding import PartitionSpec as P

LAT = 512
RANK = 16
EXPERT = ("expert_0", "expert_1")
EXPERT_DP = ("expert_0", "expert_1", "dp")
CUTS = 8
SOFTMAX_SCALE = 192.0 ** (-0.5)
ADAPTER_SCALE = 2.0
EPSILON = 1e-06
F32 = jnp.float32
BF16 = jnp.bfloat16
FAR = pl.BlockSpec(memory_space=pltpu.HBM)
WHOLE = pl.BlockSpec(memory_space=pltpu.VMEM)
SCALARS = pl.BlockSpec(memory_space=pltpu.SMEM)
GRANT = pltpu.CompilerParams(vmem_limit_bytes=16 * 2**20)


def shape(dims, dtype):
    return jax.ShapeDtypeStruct(dims, dtype)


def call(kernel, outs, flops=10**7, nbytes=10**6):
    return functools.partial(
        pl.pallas_call,
        kernel,
        out_shape=outs,
        cost_estimate=pl.CostEstimate(flops=flops, bytes_accessed=nbytes, transcendentals=0),
        compiler_params=GRANT,
    )


def exchange(rows, axis):
    return lax.all_to_all(rows, axis, split_axis=0, concat_axis=0, tiled=True)


def index(dims, dim):
    return lax.broadcasted_iota(jnp.int32, dims, dim)


def one_hot(dims, hit):
    return jnp.where(hit(index(dims, 0), index(dims, 1)), 1.0, 0.0).astype(BF16)


def dot(a, b):
    return jnp.dot(a, b, preferred_element_type=F32)


def dot_t(a, b):
    return lax.dot_general(a, b, (((1,), (1,)), ((), ())), preferred_element_type=F32)


def attend_kernel(
    lengths, ids, query, cache, *rest
):
    weights, (out, joined) = rest[:3], rest[3:5]
    lengths_here, ids_here, query_here, cache_here, weights_here, small, big, side = rest[5:]
    n, heads = query.shape[0], query.shape[1]
    firsts = [
        pltpu.make_async_copy(source, target, small.at[k])
        for k, (source, target) in enumerate(
            ((lengths, lengths_here), (ids, ids_here), (query, query_here))
        )
    ]
    rows = [pltpu.make_async_copy(cache.at[r], cache_here.at[r], big.at[r]) for r in range(n)]
    taken = [
        pltpu.make_async_copy(w, weights_here.at[k], side.at[k]) for k, w in enumerate(weights)
    ]
    given = [
        pltpu.make_async_copy(weights_here.at[k], joined.at[k], side.at[3 + k]) for k in range(3)
    ]
    for copy in (*firsts, *rows, *taken):
        copy.start()
    for copy in firsts:
        copy.wait()
    blocks = []
    lanes = out.shape[1]
    quarters = LAT // lanes
    for r in range(n):
        rows[r].wait()
        scores = dot(query_here[r], cache_here[r]) * SOFTMAX_SCALE
        valid = index(scores.shape, 1) < lengths_here[r]
        scores = jnp.where(valid, scores, -1e30)
        raised = jnp.exp(scores - jnp.max(scores, axis=1, keepdims=True))
        chances = (raised / jnp.sum(raised, axis=1, keepdims=True)).astype(BF16)
        latents = dot_t(chances, cache_here[r, :LAT, :]).astype(BF16)
        blocks += [latents[:, k * lanes : (k + 1) * lanes] for k in range(quarters)]
        if r == n - 2:
            for back, copy in zip(taken, given):
                back.wait()
                copy.start()
    held = jnp.concatenate(blocks, axis=0)

    def hit(o, c):
        owner, i = o // (2 * n), o % (2 * n)
        want = i * (quarters * heads) + (owner % quarters) * heads + owner // quarters
        return (i < n) & (c == want)

    packed = dot(one_hot((out.shape[0], held.shape[0]), hit), held)
    i = index(packed.shape, 0) % (2 * n)
    for r in range(n):
        packed = jnp.where(i == n + r, ids_here[r].astype(F32), packed)
    out[...] = packed.astype(BF16)
    for copy in given:
        copy.wait()


def attend(query, cache_t, lengths, ids, weights, owners):
    n, heads, width = query.shape
    context = cache_t.shape[2]
    lanes = heads * LAT // owners
    joined = (3, *weights[0].shape)
    return pl.pallas_call(
        attend_kernel,
        out_shape=(shape((owners * 2 * n, lanes), BF16), shape(joined, BF16)),
        in_specs=[FAR] * 7,
        out_specs=(WHOLE, FAR),
        scratch_shapes=[
            pltpu.SMEM((n,), jnp.int32),
            pltpu.SMEM((n,), jnp.int32),
            pltpu.VMEM(query.shape, BF16),
            pltpu.VMEM(cache_t.shape, BF16),
            pltpu.VMEM(joined, BF16),
            pltpu.SemaphoreType.DMA((3,)),
            pltpu.SemaphoreType.DMA((n,)),
            pltpu.SemaphoreType.DMA((6,)),
        ],
        cost_estimate=pl.CostEstimate(
            flops=4 * n * heads * width * context,
            bytes_accessed=2 * n * width * context,
            transcendentals=0,
        ),
        compiler_params=pltpu.CompilerParams(vmem_limit_bytes=56 * 2**20),
    )(lengths, ids, query, cache_t, *weights)


def lora_kernel(arrived, down, copies, pieces, numbers):
    rows = pieces.shape[0]
    lanes = arrived.shape[1]
    half = 4
    both = arrived[...]
    dims = (rows, 2 * rows)
    kept = dot(one_hot(dims, lambda o, c: c == (o // half) * 2 * half + o % half), both)
    named = dot(one_hot(dims, lambda o, c: c == (o // half) * 2 * half + half + o % half), both)
    kept = kept.astype(BF16)
    pieces[...] = kept
    numbers[...] = named.T[:8]
    total = jnp.zeros((rows, lanes), F32)
    group = index((rows, lanes), 1) // RANK
    own = named.astype(jnp.int32)
    for t in range(down.shape[1] // lanes):
        product = dot(kept, down[:, t * lanes : (t + 1) * lanes])
        total = total + jnp.where(own == group + t * (lanes // RANK), product, 0.0)
    shift = RANK
    while shift < lanes:
        total = total + pltpu.roll(total, shift, 1)
        shift *= 2
    turned = total.T[:RANK]
    for k in range(copies.shape[0]):
        copies[k] = turned


def resend_kernel(arrived, copies):
    total = jnp.sum(arrived[...], axis=0)
    for k in range(copies.shape[0]):
        copies[k] = total


def project_kernel(first, arrived, pieces, numbers, value, up, out):
    scaled = (ADAPTER_SCALE * jnp.sum(arrived[...], axis=0)).astype(BF16).astype(F32)
    number = numbers[:1].astype(jnp.int32)
    owned = up.shape[0] // RANK
    spread = [jnp.where(number == first[0] + k, scaled, 0.0) for k in range(owned)]
    spread = jnp.concatenate(spread, axis=0).T.astype(BF16)
    kept = pieces[...]
    homes, _, columns = out.shape
    rows = kept.shape[0]
    low = index((rows // 8, 8, columns), 1) < 4
    for pair in range(0, CUTS, 4):
        blocks = []
        for cut in range(pair, pair + 4):
            at = slice(cut * columns, (cut + 1) * columns)
            block = dot(kept, value[:, at]) + dot(spread, up[:, at])
            blocks.append(block.reshape(rows // 8, 8, columns))
        joined = []
        for a, b in (blocks[:2], blocks[2:]):
            even = jnp.where(low, a, pltpu.roll(b, 4, 1))
            odd = jnp.where(low, pltpu.roll(a, 4, 1), b)
            joined.append(jnp.stack([even, odd], axis=1).reshape(homes, 8, columns))
        both = jnp.concatenate(joined, axis=1)
        out[:, pair * 4 : (pair + 4) * 4, :] = both.astype(BF16)


def norm_kernel(arrived, residual, gain, stream, copies):
    flow = residual[...] + jnp.sum(arrived[...].astype(F32), axis=0)
    stream[...] = flow
    rows, columns = flow.shape
    squares = jnp.sum(flow * flow, axis=1, keepdims=True)
    for shift in (4, 8, 16):
        squares = squares + pltpu.roll(jnp.broadcast_to(squares, (rows, 128)), shift, 0)[:, :1]
    scale = lax.rsqrt(squares / (columns * CUTS) + EPSILON)
    normed = (flow * scale * gain[...]).astype(BF16)
    for k in range(copies.shape[0]):
        copies[k] = normed


def routes_kernel(routing, weights, pick, give):
    experts, tokens = routing.shape
    wide, long = tokens * CUTS, experts * CUTS
    to_expert = one_hot((long, experts), lambda o, c: o // CUTS == c)
    to_token = one_hot(
        (tokens, wide), lambda c, o: (o // (4 * CUTS) == c // 4) & (o % 4 == c % 4)
    )
    same = index((long, wide), 0) % CUTS == (index((long, wide), 1) // 4) % CUTS
    spread = dot(dot(to_expert, routing[...]).astype(BF16), to_token)
    pick[...] = jnp.where(same, spread, 0.0).astype(BF16)
    left = weights[...]
    for k in range(3):
        term = left.astype(BF16)
        left = left - term.astype(F32)
        spread = dot(dot(to_expert, term).astype(BF16), to_token)
        give[k] = jnp.where(same, spread, 0.0).astype(BF16)


def pick_kernel(pick, tokens, out):
    out[...] = dot(pick[...], tokens[...]).astype(BF16)


def give_kernel(give, rows, out):
    total = None
    for k in range(3):
        term = lax.dot_general(
            give[k], rows[...], (((0,), (0,)), ((), ())), preferred_element_type=F32
        )
        total = term if total is None else total + term
    out[...] = total.astype(BF16)


def ffn_kernel(rows, weights, out, gate_here, up_here, down_here, done):
    length, columns = rows.shape
    slots = length // CUTS
    parts = [slice(at, at + columns) for at in range(0, gate_here.shape[1], columns)]
    here = (gate_here, up_here, down_here)
    fetches = [
        [
            pltpu.make_async_copy(weights.at[k, :, part], here[k].at[:, part], done.at[k, n])
            for k in range(3)
        ]
        for n, part in enumerate(parts)
    ]
    for fetch in fetches:
        for copy in fetch:
            copy.start()
    apart = one_hot((length, length), lambda o, c: c == (o % slots) * CUTS + o // slots)
    apart = dot(apart, rows[...]).astype(BF16)
    tokens = jnp.concatenate(
        [apart[cut * slots : (cut + 1) * slots] for cut in range(CUTS)], axis=1
    )
    total = None
    for part, fetch in zip(parts, fetches):
        fetch[0].wait()
        gated = dot(tokens, gate_here[:, part])
        fetch[1].wait()
        raised = dot(tokens, up_here[:, part])
        acted = (gated / (1.0 + jnp.exp(-gated)) * raised).astype(BF16)
        fetch[2].wait()
        term = dot_t(acted, down_here[:, part])
        total = term if total is None else total + term
    result = total.astype(BF16)
    stacked = jnp.concatenate(
        [result[:, cut * columns : (cut + 1) * columns] for cut in range(CUTS)], axis=0
    )
    joint = one_hot((length, length), lambda o, c: c == (o % CUTS) * slots + o // CUTS)
    out[...] = dot(joint, stacked).astype(BF16)


def ffn(rows, weights):
    _, width, hidden = weights.shape
    slots, columns = rows.shape[0] // CUTS, rows.shape[1]
    return pl.pallas_call(
        ffn_kernel,
        out_shape=shape(rows.shape, BF16),
        in_specs=[WHOLE, FAR],
        out_specs=WHOLE,
        scratch_shapes=[pltpu.VMEM((width, hidden), BF16)] * 3
        + [pltpu.SemaphoreType.DMA((3, hidden // columns))],
        cost_estimate=pl.CostEstimate(
            flops=6 * slots * width * hidden,
            bytes_accessed=6 * width * hidden,
            transcendentals=0,
        ),
        compiler_params=pltpu.CompilerParams(vmem_limit_bytes=48 * 2**20),
    )(rows, weights)


def final_kernel(arrived, stream, out):
    total = stream[...] + jnp.sum(arrived[...].astype(F32), axis=0)
    columns = total.shape[1]
    n = out.shape[0]
    for cut in range(CUTS):
        out[:, cut * columns : (cut + 1) * columns] = total[cut * n : (cut + 1) * n].astype(BF16)


def local(
    q_latent,
    latent_cache,
    lengths,
    residual,
    adapter_ids,
    value_out,
    adapter_down,
    adapter_up_factors,
    norm_gain,
    expert_ids,
    gate_weights,
    w_gate,
    w_up,
    w_down,
):
    requests, model_width = residual.shape
    owners = lax.axis_size(EXPERT)
    dp_count = lax.axis_size("dp")
    columns = model_width // CUTS
    group = owners * requests
    owned_count = adapter_up_factors.shape[0] // RANK
    packed, joined = attend(
        q_latent,
        jnp.swapaxes(latent_cache, 1, 2),
        lengths,
        adapter_ids,
        (w_gate[0], w_up[0], w_down[0]),
        owners,
    )
    lanes = packed.shape[1]
    first = (lax.axis_index(EXPERT) * owned_count).astype(jnp.int32).reshape(1)
    packed, first = lax.optimization_barrier((packed, first))
    arrived = exchange(packed.reshape(owners, 2 * requests, lanes), EXPERT)
    arrived = arrived.reshape(owners * 2 * requests, lanes)
    side = lax.axis_size(EXPERT[0])
    copies, pieces, numbers = call(
        lora_kernel,
        (
            shape((side, RANK, group), F32),
            shape((group, lanes), BF16),
            shape((8, group), F32),
        ),
    )(in_specs=[WHOLE, WHOLE], out_specs=(WHOLE, WHOLE, WHOLE))(arrived, adapter_down)
    half = exchange(copies, EXPERT[0])
    copies = call(resend_kernel, shape((side, RANK, group), F32))(
        in_specs=[WHOLE], out_specs=WHOLE
    )(half)
    summed = exchange(copies, EXPERT[1])
    partial = call(project_kernel, shape((owners, CUTS * requests, columns), BF16))(
        in_specs=[SCALARS, WHOLE, WHOLE, WHOLE, WHOLE, WHOLE], out_specs=WHOLE
    )(first, summed, pieces, numbers, value_out, adapter_up_factors)
    at_home = exchange(partial, EXPERT)

    tokens, top_count = expert_ids.shape
    experts = owners * w_gate.shape[0]
    position = lax.axis_index("dp")
    member = expert_ids[:, :, None] == jnp.arange(experts, dtype=jnp.int32)[None, None, :]
    flat_hits = member.reshape(tokens * top_count, experts).astype(jnp.int32)
    slot_rank = jnp.sum((jnp.cumsum(flat_hits, axis=0) - 1) * flat_hits, axis=1).reshape(
        tokens, top_count
    )
    mine = member & (slot_rank == position)[:, :, None]
    routing = jnp.any(mine, axis=1).astype(BF16).T
    weights = jnp.sum(jnp.where(mine, gate_weights[:, :, None], 0.0), axis=1).T
    wide, long = tokens * CUTS, experts * CUTS
    pick, give = call(
        routes_kernel, (shape((long, wide), BF16), shape((3, long, wide), BF16))
    )(in_specs=[WHOLE, WHOLE], out_specs=(WHOLE, WHOLE))(routing, weights)

    def cut_rows(rows):
        return jnp.moveaxis(rows.reshape(-1, CUTS, columns), 1, 0)

    residual_cut = cut_rows(residual.astype(F32)).reshape(CUTS * requests, columns)
    gain_cut = jnp.broadcast_to(
        cut_rows(norm_gain.astype(F32)), (CUTS, requests, columns)
    ).reshape(CUTS * requests, columns)
    at_home, pick, give, residual_cut, gain_cut = lax.optimization_barrier(
        (at_home, pick, give, residual_cut, gain_cut)
    )
    stream, copies = call(
        norm_kernel,
        (shape((CUTS * requests, columns), F32), shape((dp_count, CUTS * requests, columns), BF16)),
    )(in_specs=[WHOLE, WHOLE, WHOLE], out_specs=(WHOLE, WHOLE))(at_home, residual_cut, gain_cut)
    column = exchange(copies, "dp").reshape(wide, columns)
    outgoing = call(pick_kernel, shape((long, columns), BF16))(
        in_specs=[WHOLE, WHOLE], out_specs=WHOLE
    )(pick, column)
    gathered = lax.all_gather(joined, "dp", axis=2, tiled=True)
    own_share = exchange(outgoing.reshape(experts, CUTS, columns), EXPERT).reshape(long, columns)
    result = ffn(own_share, gathered)
    returned = exchange(result.reshape(experts, CUTS, columns), EXPERT).reshape(long, columns)
    routed = call(give_kernel, shape((wide, columns), BF16))(
        in_specs=[WHOLE, WHOLE], out_specs=WHOLE
    )(give, returned)
    terms = exchange(routed.reshape(dp_count, CUTS * requests, columns), "dp")
    return call(final_kernel, shape((requests, model_width), BF16))(
        in_specs=[WHOLE, WHOLE], out_specs=WHOLE
    )(terms, stream)


def solution(mesh):
    split = Mesh(mesh.devices.reshape(mesh.shape["dp"], 8, 8), ("dp", "expert_0", "expert_1"))
    in_specs = (
        P(EXPERT_DP, None, None),
        P(EXPERT_DP, None, None),
        P(EXPERT_DP),
        P(EXPERT_DP, None),
        P(EXPERT_DP),
        P(EXPERT, None),
        P(EXPERT, None),
        P(EXPERT, None),
        P(),
        P(EXPERT, None),
        P(EXPERT, None),
        P(EXPERT, None, "dp"),
        P(EXPERT, None, "dp"),
        P(EXPERT, None, "dp"),
    )
    out_specs = P(EXPERT_DP, None)
    return jax.shard_map(local, mesh=split, in_specs=in_specs, out_specs=out_specs, check_vma=False)
```

```python
import functools

import jax
import jax.numpy as jnp
from jax import lax
from jax.experimental import pallas as pl
from jax.experimental.pallas import tpu as pltpu
from jax.sharding import Mesh
from jax.sharding import PartitionSpec as P

LAT = 512
RANK = 16
EXPERT = ("expert_0", "expert_1")
EXPERT_DP = ("expert_0", "expert_1", "dp")
CUTS = 8
SOFTMAX_SCALE = 192.0 ** (-0.5)
ADAPTER_SCALE = 2.0
EPSILON = 1e-06
F32 = jnp.float32
BF16 = jnp.bfloat16
FAR = pl.BlockSpec(memory_space=pltpu.HBM)
WHOLE = pl.BlockSpec(memory_space=pltpu.VMEM)
SCALARS = pl.BlockSpec(memory_space=pltpu.SMEM)
GRANT = pltpu.CompilerParams(vmem_limit_bytes=16 * 2**20)


def shape(dims, dtype):
    return jax.ShapeDtypeStruct(dims, dtype)


def call(kernel, outs, flops=10**7, nbytes=10**6):
    return functools.partial(
        pl.pallas_call,
        kernel,
        out_shape=outs,
        cost_estimate=pl.CostEstimate(flops=flops, bytes_accessed=nbytes, transcendentals=0),
        compiler_params=GRANT,
    )


def exchange(rows, axis):
    return lax.all_to_all(rows, axis, split_axis=0, concat_axis=0, tiled=True)


def index(dims, dim):
    return lax.broadcasted_iota(jnp.int32, dims, dim)


def one_hot(dims, hit):
    return jnp.where(hit(index(dims, 0), index(dims, 1)), 1.0, 0.0).astype(BF16)


def dot(a, b):
    return jnp.dot(a, b, preferred_element_type=F32)


def dot_t(a, b):
    return lax.dot_general(a, b, (((1,), (1,)), ((), ())), preferred_element_type=F32)


def attend_kernel(
    lengths, ids, query, cache, *rest
):
    weights, (out, joined) = rest[:3], rest[3:5]
    lengths_here, ids_here, query_here, cache_here, weights_here, small, big, side = rest[5:]
    n, heads = query.shape[0], query.shape[1]
    firsts = [
        pltpu.make_async_copy(source, target, small.at[k])
        for k, (source, target) in enumerate(
            ((lengths, lengths_here), (ids, ids_here), (query, query_here))
        )
    ]
    rows = [pltpu.make_async_copy(cache.at[r], cache_here.at[r], big.at[r]) for r in range(n)]
    taken = [
        pltpu.make_async_copy(w, weights_here.at[k], side.at[k]) for k, w in enumerate(weights)
    ]
    given = [
        pltpu.make_async_copy(weights_here.at[k], joined.at[k], side.at[3 + k]) for k in range(3)
    ]
    for copy in (*firsts, *rows, *taken):
        copy.start()
    for copy in firsts:
        copy.wait()
    blocks = []
    lanes = out.shape[1]
    quarters = LAT // lanes
    for r in range(n):
        rows[r].wait()
        scores = dot(query_here[r], cache_here[r]) * SOFTMAX_SCALE
        valid = index(scores.shape, 1) < lengths_here[r]
        scores = jnp.where(valid, scores, -1e30)
        raised = jnp.exp(scores - jnp.max(scores, axis=1, keepdims=True))
        chances = (raised / jnp.sum(raised, axis=1, keepdims=True)).astype(BF16)
        latents = dot_t(chances, cache_here[r, :LAT, :]).astype(BF16)
        blocks += [latents[:, k * lanes : (k + 1) * lanes] for k in range(quarters)]
        if r == n - 2:
            for back, copy in zip(taken, given):
                back.wait()
                copy.start()
    held = jnp.concatenate(blocks, axis=0)

    def hit(o, c):
        owner, i = o // (2 * n), o % (2 * n)
        want = i * (quarters * heads) + (owner % quarters) * heads + owner // quarters
        return (i < n) & (c == want)

    packed = dot(one_hot((out.shape[0], held.shape[0]), hit), held)
    i = index(packed.shape, 0) % (2 * n)
    for r in range(n):
        packed = jnp.where(i == n + r, ids_here[r].astype(F32), packed)
    out[...] = packed.astype(BF16)
    for copy in given:
        copy.wait()


def attend(query, cache_t, lengths, ids, weights, owners):
    n, heads, width = query.shape
    context = cache_t.shape[2]
    lanes = heads * LAT // owners
    joined = (3, *weights[0].shape)
    return pl.pallas_call(
        attend_kernel,
        out_shape=(shape((owners * 2 * n, lanes), BF16), shape(joined, BF16)),
        in_specs=[FAR] * 7,
        out_specs=(WHOLE, FAR),
        scratch_shapes=[
            pltpu.SMEM((n,), jnp.int32),
            pltpu.SMEM((n,), jnp.int32),
            pltpu.VMEM(query.shape, BF16),
            pltpu.VMEM(cache_t.shape, BF16),
            pltpu.VMEM(joined, BF16),
            pltpu.SemaphoreType.DMA((3,)),
            pltpu.SemaphoreType.DMA((n,)),
            pltpu.SemaphoreType.DMA((6,)),
        ],
        cost_estimate=pl.CostEstimate(
            flops=4 * n * heads * width * context,
            bytes_accessed=2 * n * width * context,
            transcendentals=0,
        ),
        compiler_params=pltpu.CompilerParams(vmem_limit_bytes=56 * 2**20),
    )(lengths, ids, query, cache_t, *weights)


def lora_kernel(arrived, down, copies, pieces, numbers):
    rows = pieces.shape[0]
    lanes = arrived.shape[1]
    half = 4
    both = arrived[...]
    dims = (rows, 2 * rows)
    kept = dot(one_hot(dims, lambda o, c: c == (o // half) * 2 * half + o % half), both)
    named = dot(one_hot(dims, lambda o, c: c == (o // half) * 2 * half + half + o % half), both)
    kept = kept.astype(BF16)
    pieces[...] = kept
    numbers[...] = named.T[:8]
    total = jnp.zeros((rows, lanes), F32)
    group = index((rows, lanes), 1) // RANK
    own = named.astype(jnp.int32)
    for t in range(down.shape[1] // lanes):
        product = dot(kept, down[:, t * lanes : (t + 1) * lanes])
        total = total + jnp.where(own == group + t * (lanes // RANK), product, 0.0)
    shift = RANK
    while shift < lanes:
        total = total + pltpu.roll(total, shift, 1)
        shift *= 2
    turned = total.T[:RANK]
    for k in range(copies.shape[0]):
        copies[k] = turned


def resend_kernel(arrived, copies):
    total = jnp.sum(arrived[...], axis=0)
    for k in range(copies.shape[0]):
        copies[k] = total


def project_kernel(first, arrived, pieces, numbers, value, up, out):
    scaled = (ADAPTER_SCALE * jnp.sum(arrived[...], axis=0)).astype(BF16).astype(F32)
    number = numbers[:1].astype(jnp.int32)
    owned = up.shape[0] // RANK
    spread = [jnp.where(number == first[0] + k, scaled, 0.0) for k in range(owned)]
    spread = jnp.concatenate(spread, axis=0).T.astype(BF16)
    kept = pieces[...]
    homes, _, columns = out.shape
    rows = kept.shape[0]
    low = index((rows // 8, 8, columns), 1) < 4
    for pair in range(0, CUTS, 4):
        blocks = []
        for cut in range(pair, pair + 4):
            at = slice(cut * columns, (cut + 1) * columns)
            block = dot(kept, value[:, at]) + dot(spread, up[:, at])
            blocks.append(block.reshape(rows // 8, 8, columns))
        joined = []
        for a, b in (blocks[:2], blocks[2:]):
            even = jnp.where(low, a, pltpu.roll(b, 4, 1))
            odd = jnp.where(low, pltpu.roll(a, 4, 1), b)
            joined.append(jnp.stack([even, odd], axis=1).reshape(homes, 8, columns))
        both = jnp.concatenate(joined, axis=1)
        out[:, pair * 4 : (pair + 4) * 4, :] = both.astype(BF16)


def norm_kernel(arrived, residual, gain, stream, copies):
    flow = residual[...] + jnp.sum(arrived[...].astype(F32), axis=0)
    stream[...] = flow
    rows, columns = flow.shape
    squares = jnp.sum(flow * flow, axis=1, keepdims=True)
    for shift in (4, 8, 16):
        squares = squares + pltpu.roll(jnp.broadcast_to(squares, (rows, 128)), shift, 0)[:, :1]
    scale = lax.rsqrt(squares / (columns * CUTS) + EPSILON)
    normed = (flow * scale * gain[...]).astype(BF16)
    for k in range(copies.shape[0]):
        copies[k] = normed


def routes_kernel(routing, weights, pick, give):
    experts, tokens = routing.shape
    wide, long = tokens * CUTS, experts * CUTS
    to_expert = one_hot((long, experts), lambda o, c: o // CUTS == c)
    to_token = one_hot(
        (tokens, wide), lambda c, o: (o // (4 * CUTS) == c // 4) & (o % 4 == c % 4)
    )
    same = index((long, wide), 0) % CUTS == (index((long, wide), 1) // 4) % CUTS
    spread = dot(dot(to_expert, routing[...]).astype(BF16), to_token)
    pick[...] = jnp.where(same, spread, 0.0).astype(BF16)
    left = weights[...]
    for k in range(3):
        term = left.astype(BF16)
        left = left - term.astype(F32)
        spread = dot(dot(to_expert, term).astype(BF16), to_token)
        give[k] = jnp.where(same, spread, 0.0).astype(BF16)


def pick_kernel(pick, tokens, out):
    out[...] = dot(pick[...], tokens[...]).astype(BF16)


def give_kernel(give, rows, out):
    total = None
    for k in range(3):
        term = lax.dot_general(
            give[k], rows[...], (((0,), (0,)), ((), ())), preferred_element_type=F32
        )
        total = term if total is None else total + term
    out[...] = total.astype(BF16)


def ffn_kernel(rows, *rest):
    shards, (out, gate, up, down, done) = rest[:-5], rest[-5:]
    length, columns = rows.shape
    slots = length // CUTS
    shards = [(w, (i,)) for w in shards for i in range(w.shape[0])]
    lanes = shards[0][0].shape[-1]
    per = gate.shape[2] // lanes
    fetches = []
    for n in range(gate.shape[0]):
        fetch = []
        for k, here in enumerate((gate, up, down)):
            for i in range(per):
                source, at = shards[n * per + i]
                fetch.append(
                    pltpu.make_async_copy(
                        source.at[(*at, k)],
                        here.at[n, :, i * lanes : (i + 1) * lanes],
                        done.at[n, k * per + i],
                    )
                )
        fetches.append(fetch)
    for fetch in fetches:
        for copy in fetch:
            copy.start()
    apart = one_hot((length, length), lambda o, c: c == (o % slots) * CUTS + o // slots)
    apart = dot(apart, rows[...]).astype(BF16)
    tokens = jnp.concatenate(
        [apart[cut * slots : (cut + 1) * slots] for cut in range(CUTS)], axis=1
    )
    total = None
    for n, fetch in enumerate(fetches):
        for copy in fetch[:per]:
            copy.wait()
        gated = dot(tokens, gate[n])
        for copy in fetch[per : 2 * per]:
            copy.wait()
        raised = dot(tokens, up[n])
        acted = (gated / (1.0 + jnp.exp(-gated)) * raised).astype(BF16)
        for copy in fetch[2 * per :]:
            copy.wait()
        term = dot_t(acted, down[n])
        total = term if total is None else total + term
    result = total.astype(BF16)
    stacked = jnp.concatenate(
        [result[:, cut * columns : (cut + 1) * columns] for cut in range(CUTS)], axis=0
    )
    joint = one_hot((length, length), lambda o, c: c == (o % CUTS) * slots + o // CUTS)
    out[...] = dot(joint, stacked).astype(BF16)


def ffn(rows, *weights):
    _, kinds, width, lanes = weights[0].shape
    hidden = lanes * sum(w.shape[0] for w in weights)
    slots = rows.shape[0] // CUTS
    per = 2
    chunk = pltpu.VMEM((hidden // (per * lanes), width, per * lanes), BF16)
    return pl.pallas_call(
        ffn_kernel,
        out_shape=shape(rows.shape, BF16),
        in_specs=[WHOLE] + [FAR] * len(weights),
        out_specs=WHOLE,
        scratch_shapes=[chunk] * 3
        + [pltpu.SemaphoreType.DMA((hidden // (per * lanes), kinds * per))],
        cost_estimate=pl.CostEstimate(
            flops=6 * slots * width * hidden,
            bytes_accessed=6 * width * hidden,
            transcendentals=0,
        ),
        compiler_params=pltpu.CompilerParams(vmem_limit_bytes=48 * 2**20),
    )(rows, *weights)


def final_kernel(arrived, stream, out):
    total = stream[...] + jnp.sum(arrived[...].astype(F32), axis=0)
    columns = total.shape[1]
    n = out.shape[0]
    for cut in range(CUTS):
        out[:, cut * columns : (cut + 1) * columns] = total[cut * n : (cut + 1) * n].astype(BF16)


def local(
    q_latent,
    latent_cache,
    lengths,
    residual,
    adapter_ids,
    value_out,
    adapter_down,
    adapter_up_factors,
    norm_gain,
    expert_ids,
    gate_weights,
    w_gate,
    w_up,
    w_down,
):
    requests, model_width = residual.shape
    owners = lax.axis_size(EXPERT)
    dp_count = lax.axis_size("dp")
    columns = model_width // CUTS
    group = owners * requests
    owned_count = adapter_up_factors.shape[0] // RANK
    packed, joined = attend(
        q_latent,
        jnp.swapaxes(latent_cache, 1, 2),
        lengths,
        adapter_ids,
        (w_gate[0], w_up[0], w_down[0]),
        owners,
    )
    lanes = packed.shape[1]
    first = (lax.axis_index(EXPERT) * owned_count).astype(jnp.int32).reshape(1)
    packed, first = lax.optimization_barrier((packed, first))
    arrived = exchange(packed.reshape(owners, 2 * requests, lanes), EXPERT)
    arrived = arrived.reshape(owners * 2 * requests, lanes)
    side = lax.axis_size(EXPERT[0])
    copies, pieces, numbers = call(
        lora_kernel,
        (
            shape((side, RANK, group), F32),
            shape((group, lanes), BF16),
            shape((8, group), F32),
        ),
    )(in_specs=[WHOLE, WHOLE], out_specs=(WHOLE, WHOLE, WHOLE))(arrived, adapter_down)
    half = exchange(copies, EXPERT[0])
    copies = call(resend_kernel, shape((side, RANK, group), F32))(
        in_specs=[WHOLE], out_specs=WHOLE
    )(half)
    summed = exchange(copies, EXPERT[1])
    partial = call(project_kernel, shape((owners, CUTS * requests, columns), BF16))(
        in_specs=[SCALARS, WHOLE, WHOLE, WHOLE, WHOLE, WHOLE], out_specs=WHOLE
    )(first, summed, pieces, numbers, value_out, adapter_up_factors)
    at_home = exchange(partial, EXPERT)

    tokens, top_count = expert_ids.shape
    experts = owners * w_gate.shape[0]
    position = lax.axis_index("dp")
    member = expert_ids[:, :, None] == jnp.arange(experts, dtype=jnp.int32)[None, None, :]
    flat_hits = member.reshape(tokens * top_count, experts).astype(jnp.int32)
    slot_rank = jnp.sum((jnp.cumsum(flat_hits, axis=0) - 1) * flat_hits, axis=1).reshape(
        tokens, top_count
    )
    mine = member & (slot_rank == position)[:, :, None]
    routing = jnp.any(mine, axis=1).astype(BF16).T
    weights = jnp.sum(jnp.where(mine, gate_weights[:, :, None], 0.0), axis=1).T
    wide, long = tokens * CUTS, experts * CUTS
    pick, give = call(
        routes_kernel, (shape((long, wide), BF16), shape((3, long, wide), BF16))
    )(in_specs=[WHOLE, WHOLE], out_specs=(WHOLE, WHOLE))(routing, weights)

    def cut_rows(rows):
        return jnp.moveaxis(rows.reshape(-1, CUTS, columns), 1, 0)

    residual_cut = cut_rows(residual.astype(F32)).reshape(CUTS * requests, columns)
    gain_cut = jnp.broadcast_to(
        cut_rows(norm_gain.astype(F32)), (CUTS, requests, columns)
    ).reshape(CUTS * requests, columns)
    at_home, pick, give, residual_cut, gain_cut = lax.optimization_barrier(
        (at_home, pick, give, residual_cut, gain_cut)
    )
    stream, copies = call(
        norm_kernel,
        (shape((CUTS * requests, columns), F32), shape((dp_count, CUTS * requests, columns), BF16)),
    )(in_specs=[WHOLE, WHOLE, WHOLE], out_specs=(WHOLE, WHOLE))(at_home, residual_cut, gain_cut)
    column = exchange(copies, "dp").reshape(wide, columns)
    outgoing = call(pick_kernel, shape((long, columns), BF16))(
        in_specs=[WHOLE, WHOLE], out_specs=WHOLE
    )(pick, column)
    gathered = lax.all_gather(joined, "dp", axis=0)
    own_share = exchange(outgoing.reshape(experts, CUTS, columns), EXPERT).reshape(long, columns)
    result = ffn(own_share, gathered)
    returned = exchange(result.reshape(experts, CUTS, columns), EXPERT).reshape(long, columns)
    routed = call(give_kernel, shape((wide, columns), BF16))(
        in_specs=[WHOLE, WHOLE], out_specs=WHOLE
    )(give, returned)
    terms = exchange(routed.reshape(dp_count, CUTS * requests, columns), "dp")
    return call(final_kernel, shape((requests, model_width), BF16))(
        in_specs=[WHOLE, WHOLE], out_specs=WHOLE
    )(terms, stream)


def solution(mesh):
    split = Mesh(mesh.devices.reshape(mesh.shape["dp"], 8, 8), ("dp", "expert_0", "expert_1"))
    in_specs = (
        P(EXPERT_DP, None, None),
        P(EXPERT_DP, None, None),
        P(EXPERT_DP),
        P(EXPERT_DP, None),
        P(EXPERT_DP),
        P(EXPERT, None),
        P(EXPERT, None),
        P(EXPERT, None),
        P(),
        P(EXPERT, None),
        P(EXPERT, None),
        P(EXPERT, None, "dp"),
        P(EXPERT, None, "dp"),
        P(EXPERT, None, "dp"),
    )
    out_specs = P(EXPERT_DP, None)
    return jax.shard_map(local, mesh=split, in_specs=in_specs, out_specs=out_specs, check_vma=False)
```

```python
import functools

import jax
import jax.numpy as jnp
from jax import lax
from jax.experimental import pallas as pl
from jax.experimental.pallas import tpu as pltpu
from jax.sharding import Mesh
from jax.sharding import PartitionSpec as P

LAT = 512
RANK = 16
EXPERT = ("expert_0", "expert_1")
EXPERT_DP = ("expert_0", "expert_1", "dp")
CUTS = 8
SOFTMAX_SCALE = 192.0 ** (-0.5)
ADAPTER_SCALE = 2.0
EPSILON = 1e-06
F32 = jnp.float32
BF16 = jnp.bfloat16
FAR = pl.BlockSpec(memory_space=pltpu.HBM)
WHOLE = pl.BlockSpec(memory_space=pltpu.VMEM)
SCALARS = pl.BlockSpec(memory_space=pltpu.SMEM)
GRANT = pltpu.CompilerParams(vmem_limit_bytes=16 * 2**20)


def shape(dims, dtype):
    return jax.ShapeDtypeStruct(dims, dtype)


def call(kernel, outs, flops=10**7, nbytes=10**6):
    return functools.partial(
        pl.pallas_call,
        kernel,
        out_shape=outs,
        cost_estimate=pl.CostEstimate(flops=flops, bytes_accessed=nbytes, transcendentals=0),
        compiler_params=GRANT,
    )


def moved(block, where):
    return lax.ppermute(block, "dp", list(enumerate(where)))


def exchange(rows, axis):
    return lax.all_to_all(rows, axis, split_axis=0, concat_axis=0, tiled=True)


def index(dims, dim):
    return lax.broadcasted_iota(jnp.int32, dims, dim)


def one_hot(dims, hit):
    return jnp.where(hit(index(dims, 0), index(dims, 1)), 1.0, 0.0).astype(BF16)


def dot(a, b):
    return jnp.dot(a, b, preferred_element_type=F32)


def dot_t(a, b):
    return lax.dot_general(a, b, (((1,), (1,)), ((), ())), preferred_element_type=F32)


def attend_kernel(
    lengths, ids, query, cache, *rest
):
    weights, (out, joined) = rest[:3], rest[3:5]
    lengths_here, ids_here, query_here, cache_here, weights_here, small, big, side = rest[5:]
    n, heads = query.shape[0], query.shape[1]
    firsts = [
        pltpu.make_async_copy(source, target, small.at[k])
        for k, (source, target) in enumerate(
            ((lengths, lengths_here), (ids, ids_here), (query, query_here))
        )
    ]
    rows = [pltpu.make_async_copy(cache.at[r], cache_here.at[r], big.at[r]) for r in range(n)]
    taken = [
        pltpu.make_async_copy(w, weights_here.at[k], side.at[k]) for k, w in enumerate(weights)
    ]
    given = [
        pltpu.make_async_copy(weights_here.at[k], joined.at[k], side.at[3 + k]) for k in range(3)
    ]
    for copy in (*firsts, *rows, *taken):
        copy.start()
    for copy in firsts:
        copy.wait()
    blocks = []
    lanes = out.shape[1]
    quarters = LAT // lanes
    for r in range(n):
        rows[r].wait()
        scores = dot(query_here[r], cache_here[r]) * SOFTMAX_SCALE
        valid = index(scores.shape, 1) < lengths_here[r]
        scores = jnp.where(valid, scores, -1e30)
        raised = jnp.exp(scores - jnp.max(scores, axis=1, keepdims=True))
        chances = (raised / jnp.sum(raised, axis=1, keepdims=True)).astype(BF16)
        latents = dot_t(chances, cache_here[r, :LAT, :]).astype(BF16)
        blocks += [latents[:, k * lanes : (k + 1) * lanes] for k in range(quarters)]
        if r == n - 2:
            for back, copy in zip(taken, given):
                back.wait()
                copy.start()
    held = jnp.concatenate(blocks, axis=0)

    def hit(o, c):
        owner, i = o // (2 * n), o % (2 * n)
        want = i * (quarters * heads) + (owner % quarters) * heads + owner // quarters
        return (i < n) & (c == want)

    packed = dot(one_hot((out.shape[0], held.shape[0]), hit), held)
    i = index(packed.shape, 0) % (2 * n)
    for r in range(n):
        packed = jnp.where(i == n + r, ids_here[r].astype(F32), packed)
    out[...] = packed.astype(BF16)
    for copy in given:
        copy.wait()


def attend(query, cache_t, lengths, ids, weights, owners):
    n, heads, width = query.shape
    context = cache_t.shape[2]
    lanes = heads * LAT // owners
    joined = (3, *weights[0].shape)
    return pl.pallas_call(
        attend_kernel,
        out_shape=(shape((owners * 2 * n, lanes), BF16), shape(joined, BF16)),
        in_specs=[FAR] * 7,
        out_specs=(WHOLE, FAR),
        scratch_shapes=[
            pltpu.SMEM((n,), jnp.int32),
            pltpu.SMEM((n,), jnp.int32),
            pltpu.VMEM(query.shape, BF16),
            pltpu.VMEM(cache_t.shape, BF16),
            pltpu.VMEM(joined, BF16),
            pltpu.SemaphoreType.DMA((3,)),
            pltpu.SemaphoreType.DMA((n,)),
            pltpu.SemaphoreType.DMA((6,)),
        ],
        cost_estimate=pl.CostEstimate(
            flops=4 * n * heads * width * context,
            bytes_accessed=2 * n * width * context,
            transcendentals=0,
        ),
        compiler_params=pltpu.CompilerParams(vmem_limit_bytes=56 * 2**20),
    )(lengths, ids, query, cache_t, *weights)


def lora_kernel(arrived, down, copies, pieces, numbers):
    rows = pieces.shape[0]
    lanes = arrived.shape[1]
    half = 4
    both = arrived[...]
    dims = (rows, 2 * rows)
    kept = dot(one_hot(dims, lambda o, c: c == (o // half) * 2 * half + o % half), both)
    named = dot(one_hot(dims, lambda o, c: c == (o // half) * 2 * half + half + o % half), both)
    kept = kept.astype(BF16)
    pieces[...] = kept
    numbers[...] = named.T[:8]
    total = jnp.zeros((rows, lanes), F32)
    group = index((rows, lanes), 1) // RANK
    own = named.astype(jnp.int32)
    for t in range(down.shape[1] // lanes):
        product = dot(kept, down[:, t * lanes : (t + 1) * lanes])
        total = total + jnp.where(own == group + t * (lanes // RANK), product, 0.0)
    shift = RANK
    while shift < lanes:
        total = total + pltpu.roll(total, shift, 1)
        shift *= 2
    turned = total.T[:RANK]
    for k in range(copies.shape[0]):
        copies[k] = turned


def resend_kernel(arrived, copies):
    total = jnp.sum(arrived[...], axis=0)
    for k in range(copies.shape[0]):
        copies[k] = total


def project_kernel(first, arrived, pieces, numbers, value, up, out):
    scaled = (ADAPTER_SCALE * jnp.sum(arrived[...], axis=0)).astype(BF16).astype(F32)
    number = numbers[:1].astype(jnp.int32)
    owned = up.shape[0] // RANK
    spread = [jnp.where(number == first[0] + k, scaled, 0.0) for k in range(owned)]
    spread = jnp.concatenate(spread, axis=0).T.astype(BF16)
    kept = pieces[...]
    homes, _, columns = out.shape
    rows = kept.shape[0]
    low = index((rows // 8, 8, columns), 1) < 4
    for pair in range(0, CUTS, 4):
        blocks = []
        for cut in range(pair, pair + 4):
            at = slice(cut * columns, (cut + 1) * columns)
            block = dot(kept, value[:, at]) + dot(spread, up[:, at])
            blocks.append(block.reshape(rows // 8, 8, columns))
        joined = []
        for a, b in (blocks[:2], blocks[2:]):
            even = jnp.where(low, a, pltpu.roll(b, 4, 1))
            odd = jnp.where(low, pltpu.roll(a, 4, 1), b)
            joined.append(jnp.stack([even, odd], axis=1).reshape(homes, 8, columns))
        both = jnp.concatenate(joined, axis=1)
        out[:, pair * 4 : (pair + 4) * 4, :] = both.astype(BF16)


def norm_kernel(arrived, residual, gain, stream, copies):
    flow = residual[...] + jnp.sum(arrived[...].astype(F32), axis=0)
    stream[...] = flow
    rows, columns = flow.shape
    squares = jnp.sum(flow * flow, axis=1, keepdims=True)
    for shift in (4, 8, 16):
        squares = squares + pltpu.roll(jnp.broadcast_to(squares, (rows, 128)), shift, 0)[:, :1]
    scale = lax.rsqrt(squares / (columns * CUTS) + EPSILON)
    normed = (flow * scale * gain[...]).astype(BF16)
    for k in range(copies.shape[0]):
        copies[k] = normed


def routes_kernel(routing, weights, pick, give):
    experts, tokens = routing.shape
    wide, long = tokens * CUTS, experts * CUTS
    to_expert = one_hot((long, experts), lambda o, c: o // CUTS == c)
    to_token = one_hot(
        (tokens, wide), lambda c, o: (o // (4 * CUTS) == c // 4) & (o % 4 == c % 4)
    )
    same = index((long, wide), 0) % CUTS == (index((long, wide), 1) // 4) % CUTS
    spread = dot(dot(to_expert, routing[...]).astype(BF16), to_token)
    pick[...] = jnp.where(same, spread, 0.0).astype(BF16)
    left = weights[...]
    for k in range(3):
        term = left.astype(BF16)
        left = left - term.astype(F32)
        spread = dot(dot(to_expert, term).astype(BF16), to_token)
        give[k] = jnp.where(same, spread, 0.0).astype(BF16)


def pick_kernel(pick, tokens, out):
    out[...] = dot(pick[...], tokens[...]).astype(BF16)


def give_kernel(give, rows, out):
    total = None
    for k in range(3):
        term = lax.dot_general(
            give[k], rows[...], (((0,), (0,)), ((), ())), preferred_element_type=F32
        )
        total = term if total is None else total + term
    out[...] = total.astype(BF16)


def ffn_kernel(rows, *rest):
    shards, (out, gate, up, down, done) = rest[:-5], rest[-5:]
    length, columns = rows.shape
    slots = length // CUTS
    shards = [(w, (i,)) for w in shards for i in range(w.shape[0])]
    lanes = shards[0][0].shape[-1]
    per = gate.shape[2] // lanes
    fetches = []
    for n in range(gate.shape[0]):
        fetch = []
        for k, here in enumerate((gate, up, down)):
            for i in range(per):
                source, at = shards[n * per + i]
                fetch.append(
                    pltpu.make_async_copy(
                        source.at[(*at, k)],
                        here.at[n, :, i * lanes : (i + 1) * lanes],
                        done.at[n, k * per + i],
                    )
                )
        fetches.append(fetch)
    for fetch in fetches:
        for copy in fetch:
            copy.start()
    apart = one_hot((length, length), lambda o, c: c == (o % slots) * CUTS + o // slots)
    apart = dot(apart, rows[...]).astype(BF16)
    tokens = jnp.concatenate(
        [apart[cut * slots : (cut + 1) * slots] for cut in range(CUTS)], axis=1
    )
    total = None
    for n, fetch in enumerate(fetches):
        for copy in fetch[:per]:
            copy.wait()
        gated = dot(tokens, gate[n])
        for copy in fetch[per : 2 * per]:
            copy.wait()
        raised = dot(tokens, up[n])
        acted = (gated / (1.0 + jnp.exp(-gated)) * raised).astype(BF16)
        for copy in fetch[2 * per :]:
            copy.wait()
        term = dot_t(acted, down[n])
        total = term if total is None else total + term
    result = total.astype(BF16)
    stacked = jnp.concatenate(
        [result[:, cut * columns : (cut + 1) * columns] for cut in range(CUTS)], axis=0
    )
    joint = one_hot((length, length), lambda o, c: c == (o % CUTS) * slots + o // CUTS)
    out[...] = dot(joint, stacked).astype(BF16)


def ffn(rows, *weights):
    _, kinds, width, lanes = weights[0].shape
    hidden = lanes * sum(w.shape[0] for w in weights)
    slots = rows.shape[0] // CUTS
    per = 2
    chunk = pltpu.VMEM((hidden // (per * lanes), width, per * lanes), BF16)
    return pl.pallas_call(
        ffn_kernel,
        out_shape=shape(rows.shape, BF16),
        in_specs=[WHOLE] + [FAR] * len(weights),
        out_specs=WHOLE,
        scratch_shapes=[chunk] * 3
        + [pltpu.SemaphoreType.DMA((hidden // (per * lanes), kinds * per))],
        cost_estimate=pl.CostEstimate(
            flops=6 * slots * width * hidden,
            bytes_accessed=6 * width * hidden,
            transcendentals=0,
        ),
        compiler_params=pltpu.CompilerParams(vmem_limit_bytes=52 * 2**20),
    )(rows, *weights)


def final_kernel(arrived, stream, out):
    total = stream[...] + jnp.sum(arrived[...].astype(F32), axis=0)
    columns = total.shape[1]
    n = out.shape[0]
    for cut in range(CUTS):
        out[:, cut * columns : (cut + 1) * columns] = total[cut * n : (cut + 1) * n].astype(BF16)


def local(
    q_latent,
    latent_cache,
    lengths,
    residual,
    adapter_ids,
    value_out,
    adapter_down,
    adapter_up_factors,
    norm_gain,
    expert_ids,
    gate_weights,
    w_gate,
    w_up,
    w_down,
):
    requests, model_width = residual.shape
    owners = lax.axis_size(EXPERT)
    dp_count = lax.axis_size("dp")
    columns = model_width // CUTS
    group = owners * requests
    owned_count = adapter_up_factors.shape[0] // RANK
    packed, joined = attend(
        q_latent,
        jnp.swapaxes(latent_cache, 1, 2),
        lengths,
        adapter_ids,
        (w_gate[0], w_up[0], w_down[0]),
        owners,
    )
    lanes = packed.shape[1]
    first = (lax.axis_index(EXPERT) * owned_count).astype(jnp.int32).reshape(1)
    packed, first = lax.optimization_barrier((packed, first))
    arrived = exchange(packed.reshape(owners, 2 * requests, lanes), EXPERT)
    ups = [(d + 2) % dp_count for d in range(dp_count)]
    downs = [(d - 2) % dp_count for d in range(dp_count)]
    swap = [d ^ 1 for d in range(dp_count)]
    from_below = moved(joined, ups)
    from_above = moved(joined, downs)
    shards = [joined, from_below, from_above]
    own_swapped = moved(joined, swap)
    arrived, own_swapped = lax.optimization_barrier((arrived, own_swapped))
    shards.append(own_swapped)
    on = jnp.where(lax.axis_index("dp") % 2 == 0, from_above, from_below)
    relayed = [downs[d] if d % 2 == 0 else ups[d] for d in range(dp_count)]
    opposite = moved(on, relayed)
    below_swapped = moved(from_below, swap)
    above_swapped = moved(from_above, swap)
    opposite_swapped = moved(opposite, swap)
    arrived = arrived.reshape(owners * 2 * requests, lanes)
    side = lax.axis_size(EXPERT[0])
    copies, pieces, numbers = call(
        lora_kernel,
        (
            shape((side, RANK, group), F32),
            shape((group, lanes), BF16),
            shape((8, group), F32),
        ),
    )(in_specs=[WHOLE, WHOLE], out_specs=(WHOLE, WHOLE, WHOLE))(arrived, adapter_down)
    half = exchange(copies, EXPERT[0])
    copies = call(resend_kernel, shape((side, RANK, group), F32))(
        in_specs=[WHOLE], out_specs=WHOLE
    )(half)
    summed = exchange(copies, EXPERT[1])
    partial = call(project_kernel, pltpu.HBM((owners, CUTS * requests, columns), BF16))(
        in_specs=[SCALARS, WHOLE, WHOLE, WHOLE, WHOLE, WHOLE], out_specs=WHOLE
    )(first, summed, pieces, numbers, value_out, adapter_up_factors)
    at_home = exchange(partial, EXPERT)

    tokens, top_count = expert_ids.shape
    experts = owners * w_gate.shape[0]
    position = lax.axis_index("dp")
    member = expert_ids[:, :, None] == jnp.arange(experts, dtype=jnp.int32)[None, None, :]
    flat_hits = member.reshape(tokens * top_count, experts).astype(jnp.int32)
    slot_rank = jnp.sum((jnp.cumsum(flat_hits, axis=0) - 1) * flat_hits, axis=1).reshape(
        tokens, top_count
    )
    mine = member & (slot_rank == position)[:, :, None]
    routing = jnp.any(mine, axis=1).astype(BF16).T
    weights = jnp.sum(jnp.where(mine, gate_weights[:, :, None], 0.0), axis=1).T
    wide, long = tokens * CUTS, experts * CUTS
    pick, give = call(
        routes_kernel, (shape((long, wide), BF16), shape((3, long, wide), BF16))
    )(in_specs=[WHOLE, WHOLE], out_specs=(WHOLE, WHOLE))(routing, weights)

    def cut_rows(rows):
        return jnp.moveaxis(rows.reshape(-1, CUTS, columns), 1, 0)

    residual_cut = cut_rows(residual.astype(F32)).reshape(CUTS * requests, columns)
    gain_cut = jnp.broadcast_to(
        cut_rows(norm_gain.astype(F32)), (CUTS, requests, columns)
    ).reshape(CUTS * requests, columns)
    at_home, pick, give, residual_cut, gain_cut, below_swapped, above_swapped = (
        lax.optimization_barrier(
            (at_home, pick, give, residual_cut, gain_cut, below_swapped, above_swapped)
        )
    )
    shards += [opposite, below_swapped, above_swapped, opposite_swapped]
    stream, copies = call(
        norm_kernel,
        (shape((CUTS * requests, columns), F32), shape((dp_count, CUTS * requests, columns), BF16)),
    )(in_specs=[WHOLE, WHOLE, WHOLE], out_specs=(WHOLE, WHOLE))(at_home, residual_cut, gain_cut)
    column = exchange(copies, "dp").reshape(wide, columns)
    outgoing = call(pick_kernel, pltpu.HBM((long, columns), BF16))(
        in_specs=[WHOLE, WHOLE], out_specs=WHOLE
    )(pick, column)
    own_share = exchange(outgoing.reshape(experts, CUTS, columns), EXPERT)
    own_share = own_share.reshape(long, columns)
    result = ffn(own_share, *(w[None] for w in shards))
    returned = exchange(result.reshape(experts, CUTS, columns), EXPERT).reshape(long, columns)
    routed = call(give_kernel, shape((wide, columns), BF16))(
        in_specs=[WHOLE, WHOLE], out_specs=WHOLE
    )(give, returned)
    terms = exchange(routed.reshape(dp_count, CUTS * requests, columns), "dp")
    return call(final_kernel, shape((requests, model_width), BF16))(
        in_specs=[WHOLE, WHOLE], out_specs=WHOLE
    )(terms, stream)


def solution(mesh):
    split = Mesh(mesh.devices.reshape(mesh.shape["dp"], 8, 8), ("dp", "expert_0", "expert_1"))
    in_specs = (
        P(EXPERT_DP, None, None),
        P(EXPERT_DP, None, None),
        P(EXPERT_DP),
        P(EXPERT_DP, None),
        P(EXPERT_DP),
        P(EXPERT, None),
        P(EXPERT, None),
        P(EXPERT, None),
        P(),
        P(EXPERT, None),
        P(EXPERT, None),
        P(EXPERT, None, "dp"),
        P(EXPERT, None, "dp"),
        P(EXPERT, None, "dp"),
    )
    out_specs = P(EXPERT_DP, None)
    return jax.shard_map(local, mesh=split, in_specs=in_specs, out_specs=out_specs, check_vma=False)
```

```python
import functools

import jax
import jax.numpy as jnp
from jax import lax
from jax.experimental import pallas as pl
from jax.experimental.pallas import tpu as pltpu
from jax.sharding import Mesh
from jax.sharding import PartitionSpec as P

LAT = 512
RANK = 16
EXPERT = ("expert_0", "expert_1")
EXPERT_DP = ("expert_0", "expert_1", "dp")
CUTS = 8
SOFTMAX_SCALE = 192.0 ** (-0.5)
ADAPTER_SCALE = 2.0
EPSILON = 1e-06
F32 = jnp.float32
BF16 = jnp.bfloat16
FAR = pl.BlockSpec(memory_space=pltpu.HBM)
WHOLE = pl.BlockSpec(memory_space=pltpu.VMEM)
SCALARS = pl.BlockSpec(memory_space=pltpu.SMEM)
GRANT = pltpu.CompilerParams(vmem_limit_bytes=16 * 2**20)


def shape(dims, dtype):
    return jax.ShapeDtypeStruct(dims, dtype)


def call(kernel, outs, flops=10**7, nbytes=10**6):
    return functools.partial(
        pl.pallas_call,
        kernel,
        out_shape=outs,
        cost_estimate=pl.CostEstimate(flops=flops, bytes_accessed=nbytes, transcendentals=0),
        compiler_params=GRANT,
    )


def moved(block, where):
    return lax.ppermute(block, "dp", list(enumerate(where)))


def exchange(rows, axis):
    return lax.all_to_all(rows, axis, split_axis=0, concat_axis=0, tiled=True)


def index(dims, dim):
    return lax.broadcasted_iota(jnp.int32, dims, dim)


def one_hot(dims, hit):
    return jnp.where(hit(index(dims, 0), index(dims, 1)), 1.0, 0.0).astype(BF16)


def dot(a, b):
    return jnp.dot(a, b, preferred_element_type=F32)


def dot_t(a, b):
    return lax.dot_general(a, b, (((1,), (1,)), ((), ())), preferred_element_type=F32)


def attend_kernel(
    lengths, ids, query, cache, *rest
):
    weights, (out, joined) = rest[:3], rest[3:5]
    lengths_here, ids_here, query_here, cache_here, weights_here, small, big, side = rest[5:]
    n, heads = query.shape[0], query.shape[1]
    firsts = [
        pltpu.make_async_copy(source, target, small.at[k])
        for k, (source, target) in enumerate(
            ((lengths, lengths_here), (ids, ids_here), (query, query_here))
        )
    ]
    rows = [pltpu.make_async_copy(cache.at[r], cache_here.at[r], big.at[r]) for r in range(n)]
    taken = [
        pltpu.make_async_copy(w, weights_here.at[k], side.at[k]) for k, w in enumerate(weights)
    ]
    given = [
        pltpu.make_async_copy(weights_here.at[k], joined.at[k], side.at[3 + k]) for k in range(3)
    ]
    for copy in (*firsts, *rows, *taken):
        copy.start()
    for copy in firsts:
        copy.wait()
    blocks = []
    lanes = out.shape[1]
    quarters = LAT // lanes
    for r in range(n):
        rows[r].wait()
        scores = dot(query_here[r], cache_here[r]) * SOFTMAX_SCALE
        valid = index(scores.shape, 1) < lengths_here[r]
        scores = jnp.where(valid, scores, -1e30)
        raised = jnp.exp(scores - jnp.max(scores, axis=1, keepdims=True))
        chances = (raised / jnp.sum(raised, axis=1, keepdims=True)).astype(BF16)
        latents = dot_t(chances, cache_here[r, :LAT, :]).astype(BF16)
        blocks += [latents[:, k * lanes : (k + 1) * lanes] for k in range(quarters)]
        if r == n - 2:
            for back, copy in zip(taken, given):
                back.wait()
                copy.start()
    held = jnp.concatenate(blocks, axis=0)

    def hit(o, c):
        owner, i = o // (2 * n), o % (2 * n)
        want = i * (quarters * heads) + (owner % quarters) * heads + owner // quarters
        return (i < n) & (c == want)

    packed = dot(one_hot((out.shape[0], held.shape[0]), hit), held)
    i = index(packed.shape, 0) % (2 * n)
    for r in range(n):
        packed = jnp.where(i == n + r, ids_here[r].astype(F32), packed)
    out[...] = packed.astype(BF16)
    for copy in given:
        copy.wait()


def attend(query, cache_t, lengths, ids, weights, owners):
    n, heads, width = query.shape
    context = cache_t.shape[2]
    lanes = heads * LAT // owners
    joined = (3, *weights[0].shape)
    return pl.pallas_call(
        attend_kernel,
        out_shape=(shape((owners * 2 * n, lanes), BF16), shape(joined, BF16)),
        in_specs=[FAR] * 7,
        out_specs=(WHOLE, FAR),
        scratch_shapes=[
            pltpu.SMEM((n,), jnp.int32),
            pltpu.SMEM((n,), jnp.int32),
            pltpu.VMEM(query.shape, BF16),
            pltpu.VMEM(cache_t.shape, BF16),
            pltpu.VMEM(joined, BF16),
            pltpu.SemaphoreType.DMA((3,)),
            pltpu.SemaphoreType.DMA((n,)),
            pltpu.SemaphoreType.DMA((6,)),
        ],
        cost_estimate=pl.CostEstimate(
            flops=4 * n * heads * width * context,
            bytes_accessed=2 * n * width * context,
            transcendentals=0,
        ),
        compiler_params=pltpu.CompilerParams(vmem_limit_bytes=56 * 2**20),
    )(lengths, ids, query, cache_t, *weights)


def lora_kernel(arrived, down, copies, pieces, numbers):
    rows = pieces.shape[0]
    lanes = arrived.shape[1]
    half = 4
    both = arrived[...]
    dims = (rows, 2 * rows)
    kept = dot(one_hot(dims, lambda o, c: c == (o // half) * 2 * half + o % half), both)
    named = dot(one_hot(dims, lambda o, c: c == (o // half) * 2 * half + half + o % half), both)
    kept = kept.astype(BF16)
    pieces[...] = kept
    numbers[...] = named.T[:8]
    total = jnp.zeros((rows, lanes), F32)
    group = index((rows, lanes), 1) // RANK
    own = named.astype(jnp.int32)
    for t in range(down.shape[1] // lanes):
        product = dot(kept, down[:, t * lanes : (t + 1) * lanes])
        total = total + jnp.where(own == group + t * (lanes // RANK), product, 0.0)
    shift = RANK
    while shift < lanes:
        total = total + pltpu.roll(total, shift, 1)
        shift *= 2
    turned = total.T[:RANK]
    for k in range(copies.shape[0]):
        copies[k] = turned


def resend_kernel(arrived, copies):
    total = jnp.sum(arrived[...], axis=0)
    for k in range(copies.shape[0]):
        copies[k] = total


def project_kernel(first, arrived, pieces, numbers, value, up, out):
    scaled = (ADAPTER_SCALE * jnp.sum(arrived[...], axis=0)).astype(BF16).astype(F32)
    number = numbers[:1].astype(jnp.int32)
    owned = up.shape[0] // RANK
    spread = [jnp.where(number == first[0] + k, scaled, 0.0) for k in range(owned)]
    spread = jnp.concatenate(spread, axis=0).T.astype(BF16)
    kept = pieces[...]
    homes, _, columns = out.shape
    rows = kept.shape[0]
    low = index((rows // 8, 8, columns), 1) < 4
    for pair in range(0, CUTS, 4):
        blocks = []
        for cut in range(pair, pair + 4):
            at = slice(cut * columns, (cut + 1) * columns)
            block = dot(kept, value[:, at]) + dot(spread, up[:, at])
            blocks.append(block.reshape(rows // 8, 8, columns))
        joined = []
        for a, b in (blocks[:2], blocks[2:]):
            even = jnp.where(low, a, pltpu.roll(b, 4, 1))
            odd = jnp.where(low, pltpu.roll(a, 4, 1), b)
            joined.append(jnp.stack([even, odd], axis=1).reshape(homes, 8, columns))
        both = jnp.concatenate(joined, axis=1)
        out[:, pair * 4 : (pair + 4) * 4, :] = both.astype(BF16)


def norm_kernel(arrived, residual, gain, stream, copies):
    flow = residual[...] + jnp.sum(arrived[...].astype(F32), axis=0)
    stream[...] = flow
    rows, columns = flow.shape
    squares = jnp.sum(flow * flow, axis=1, keepdims=True)
    for shift in (4, 8, 16):
        squares = squares + pltpu.roll(jnp.broadcast_to(squares, (rows, 128)), shift, 0)[:, :1]
    scale = lax.rsqrt(squares / (columns * CUTS) + EPSILON)
    normed = (flow * scale * gain[...]).astype(BF16)
    for k in range(copies.shape[0]):
        copies[k] = normed


def routes_kernel(routing, weights, pick, give):
    experts, tokens = routing.shape
    wide, long = tokens * CUTS, experts * CUTS
    to_expert = one_hot((long, experts), lambda o, c: o // CUTS == c)
    to_token = one_hot(
        (tokens, wide), lambda c, o: (o // (4 * CUTS) == c // 4) & (o % 4 == c % 4)
    )
    same = index((long, wide), 0) % CUTS == (index((long, wide), 1) // 4) % CUTS
    spread = dot(dot(to_expert, routing[...]).astype(BF16), to_token)
    pick[...] = jnp.where(same, spread, 0.0).astype(BF16)
    left = weights[...]
    for k in range(3):
        term = left.astype(BF16)
        left = left - term.astype(F32)
        spread = dot(dot(to_expert, term).astype(BF16), to_token)
        give[k] = jnp.where(same, spread, 0.0).astype(BF16)


def pick_kernel(pick, tokens, out):
    out[...] = dot(pick[...], tokens[...]).astype(BF16)


def give_kernel(give, rows, out):
    total = None
    for k in range(3):
        term = lax.dot_general(
            give[k], rows[...], (((0,), (0,)), ((), ())), preferred_element_type=F32
        )
        total = term if total is None else total + term
    out[...] = total.astype(BF16)


def ffn_kernel(rows, *rest):
    shards, (out, gate, up, down, done) = rest[:-5], rest[-5:]
    length, columns = rows.shape
    slots = length // CUTS
    shards = [(w, (i,)) for w in shards for i in range(w.shape[0])]
    lanes = shards[0][0].shape[-1]
    per = gate.shape[2] // lanes
    fetches = []
    for n in range(gate.shape[0]):
        fetch = []
        for k, here in enumerate((gate, up, down)):
            for i in range(per):
                source, at = shards[n * per + i]
                fetch.append(
                    pltpu.make_async_copy(
                        source.at[(*at, k)],
                        here.at[n, :, i * lanes : (i + 1) * lanes],
                        done.at[n, k * per + i],
                    )
                )
        fetches.append(fetch)
    for fetch in fetches:
        for copy in fetch:
            copy.start()
    apart = one_hot((length, length), lambda o, c: c == (o % slots) * CUTS + o // slots)
    apart = dot(apart, rows[...]).astype(BF16)
    tokens = jnp.concatenate(
        [apart[cut * slots : (cut + 1) * slots] for cut in range(CUTS)], axis=1
    )
    total = None
    for n, fetch in enumerate(fetches):
        for copy in fetch[:per]:
            copy.wait()
        gated = dot(tokens, gate[n])
        for copy in fetch[per : 2 * per]:
            copy.wait()
        raised = dot(tokens, up[n])
        acted = (gated / (1.0 + jnp.exp(-gated)) * raised).astype(BF16)
        for copy in fetch[2 * per :]:
            copy.wait()
        term = dot_t(acted, down[n])
        total = term if total is None else total + term
    result = total.astype(BF16)
    stacked = jnp.concatenate(
        [result[:, cut * columns : (cut + 1) * columns] for cut in range(CUTS)], axis=0
    )
    joint = one_hot((length, length), lambda o, c: c == (o % CUTS) * slots + o // CUTS)
    out[...] = dot(joint, stacked).astype(BF16)


def ffn(rows, *weights):
    _, kinds, width, lanes = weights[0].shape
    hidden = lanes * sum(w.shape[0] for w in weights)
    slots = rows.shape[0] // CUTS
    per = 2
    chunk = pltpu.VMEM((hidden // (per * lanes), width, per * lanes), BF16)
    return pl.pallas_call(
        ffn_kernel,
        out_shape=shape(rows.shape, BF16),
        in_specs=[WHOLE] + [FAR] * len(weights),
        out_specs=WHOLE,
        scratch_shapes=[chunk] * 3
        + [pltpu.SemaphoreType.DMA((hidden // (per * lanes), kinds * per))],
        cost_estimate=pl.CostEstimate(
            flops=6 * slots * width * hidden,
            bytes_accessed=6 * width * hidden,
            transcendentals=0,
        ),
        compiler_params=pltpu.CompilerParams(vmem_limit_bytes=51 * 2**20),
    )(rows, *weights)


def final_kernel(arrived, stream, out):
    total = stream[...] + jnp.sum(arrived[...].astype(F32), axis=0)
    columns = total.shape[1]
    n = out.shape[0]
    for cut in range(CUTS):
        out[:, cut * columns : (cut + 1) * columns] = total[cut * n : (cut + 1) * n].astype(BF16)


def local(
    q_latent,
    latent_cache,
    lengths,
    residual,
    adapter_ids,
    value_out,
    adapter_down,
    adapter_up_factors,
    norm_gain,
    expert_ids,
    gate_weights,
    w_gate,
    w_up,
    w_down,
):
    requests, model_width = residual.shape
    owners = lax.axis_size(EXPERT)
    dp_count = lax.axis_size("dp")
    columns = model_width // CUTS
    group = owners * requests
    owned_count = adapter_up_factors.shape[0] // RANK
    packed, joined = attend(
        q_latent,
        jnp.swapaxes(latent_cache, 1, 2),
        lengths,
        adapter_ids,
        (w_gate[0], w_up[0], w_down[0]),
        owners,
    )
    lanes = packed.shape[1]
    first = (lax.axis_index(EXPERT) * owned_count).astype(jnp.int32).reshape(1)
    packed, first = lax.optimization_barrier((packed, first))
    arrived = exchange(packed.reshape(owners, 2 * requests, lanes), EXPERT)
    ups = [(d + 2) % dp_count for d in range(dp_count)]
    downs = [(d - 2) % dp_count for d in range(dp_count)]
    swap = [d ^ 1 for d in range(dp_count)]
    from_below = moved(joined, ups)
    from_above = moved(joined, downs)
    shards = [joined, from_below, from_above]
    own_swapped = moved(joined, swap)
    on = jnp.where(lax.axis_index("dp") % 2 == 0, from_above, from_below)
    relayed = [downs[d] if d % 2 == 0 else ups[d] for d in range(dp_count)]
    opposite = moved(on, relayed)
    below_swapped = moved(from_below, swap)
    above_swapped = moved(from_above, swap)
    opposite_swapped = moved(opposite, swap)
    arrived = arrived.reshape(owners * 2 * requests, lanes)
    side = lax.axis_size(EXPERT[0])
    copies, pieces, numbers = call(
        lora_kernel,
        (
            shape((side, RANK, group), F32),
            shape((group, lanes), BF16),
            shape((8, group), F32),
        ),
    )(in_specs=[WHOLE, WHOLE], out_specs=(WHOLE, WHOLE, WHOLE))(arrived, adapter_down)
    half = exchange(copies, EXPERT[0])
    copies = call(resend_kernel, shape((side, RANK, group), F32))(
        in_specs=[WHOLE], out_specs=WHOLE
    )(half)
    summed = exchange(copies, EXPERT[1])
    partial = call(project_kernel, pltpu.HBM((owners, CUTS * requests, columns), BF16))(
        in_specs=[SCALARS, WHOLE, WHOLE, WHOLE, WHOLE, WHOLE], out_specs=WHOLE
    )(first, summed, pieces, numbers, value_out, adapter_up_factors)
    at_home = exchange(partial, EXPERT)

    tokens, top_count = expert_ids.shape
    experts = owners * w_gate.shape[0]
    position = lax.axis_index("dp")
    member = expert_ids[:, :, None] == jnp.arange(experts, dtype=jnp.int32)[None, None, :]
    flat_hits = member.reshape(tokens * top_count, experts).astype(jnp.int32)
    slot_rank = jnp.sum((jnp.cumsum(flat_hits, axis=0) - 1) * flat_hits, axis=1).reshape(
        tokens, top_count
    )
    mine = member & (slot_rank == position)[:, :, None]
    routing = jnp.any(mine, axis=1).astype(BF16).T
    weights = jnp.sum(jnp.where(mine, gate_weights[:, :, None], 0.0), axis=1).T
    wide, long = tokens * CUTS, experts * CUTS
    pick, give = call(
        routes_kernel, (shape((long, wide), BF16), shape((3, long, wide), BF16))
    )(in_specs=[WHOLE, WHOLE], out_specs=(WHOLE, WHOLE))(routing, weights)

    def cut_rows(rows):
        return jnp.moveaxis(rows.reshape(-1, CUTS, columns), 1, 0)

    residual_cut = cut_rows(residual.astype(F32)).reshape(CUTS * requests, columns)
    gain_cut = jnp.broadcast_to(
        cut_rows(norm_gain.astype(F32)), (CUTS, requests, columns)
    ).reshape(CUTS * requests, columns)
    swapped = (own_swapped, below_swapped, above_swapped)
    at_home, pick, give, residual_cut, gain_cut, *swapped = lax.optimization_barrier(
        (at_home, pick, give, residual_cut, gain_cut, *swapped)
    )
    shards += [opposite, *swapped, opposite_swapped]
    stream, copies = call(
        norm_kernel,
        (shape((CUTS * requests, columns), F32), shape((dp_count, CUTS * requests, columns), BF16)),
    )(in_specs=[WHOLE, WHOLE, WHOLE], out_specs=(WHOLE, WHOLE))(at_home, residual_cut, gain_cut)
    column = exchange(copies, "dp").reshape(wide, columns)
    outgoing = call(pick_kernel, pltpu.HBM((long, columns), BF16))(
        in_specs=[WHOLE, WHOLE], out_specs=WHOLE
    )(pick, column)
    own_share = exchange(outgoing.reshape(experts, CUTS, columns), EXPERT)
    own_share = own_share.reshape(long, columns)
    result = ffn(own_share, *(w[None] for w in shards))
    returned = exchange(result.reshape(experts, CUTS, columns), EXPERT).reshape(long, columns)
    routed = call(give_kernel, shape((wide, columns), BF16))(
        in_specs=[WHOLE, WHOLE], out_specs=WHOLE
    )(give, returned)
    terms = exchange(routed.reshape(dp_count, CUTS * requests, columns), "dp")
    return call(final_kernel, shape((requests, model_width), BF16))(
        in_specs=[WHOLE, WHOLE], out_specs=WHOLE
    )(terms, stream)


def solution(mesh):
    split = Mesh(mesh.devices.reshape(mesh.shape["dp"], 8, 8), ("dp", "expert_0", "expert_1"))
    in_specs = (
        P(EXPERT_DP, None, None),
        P(EXPERT_DP, None, None),
        P(EXPERT_DP),
        P(EXPERT_DP, None),
        P(EXPERT_DP),
        P(EXPERT, None),
        P(EXPERT, None),
        P(EXPERT, None),
        P(),
        P(EXPERT, None),
        P(EXPERT, None),
        P(EXPERT, None, "dp"),
        P(EXPERT, None, "dp"),
        P(EXPERT, None, "dp"),
    )
    out_specs = P(EXPERT_DP, None)
    return jax.shard_map(local, mesh=split, in_specs=in_specs, out_specs=out_specs, check_vma=False)
```
